32 devices in a mesh: groups: 2 (over x), seq: 8 (over z, y), dec: 2 (over core).
Axes of the slice: x: 2, y: 2, z: 4, core: 2. Of those that a mesh axis runs over, the one named last changes fastest.
Arguments:
- tokens: bfloat16 [2048, 4096], P(('groups', 'seq')), parts along dimension 0, may hold values from -64 to 64
- norm_gain: float32 [4096], replicated, may hold values from 0.25 to 1.75
- w_query: bfloat16 [4096, 2048], P('seq', 'dec'), may hold values from -0.140625 to 0.140625
- w_key: bfloat16 [4096, 512], P('seq', 'dec'), may hold values from -0.140625 to 0.140625
- w_value: bfloat16 [4096, 512], P('seq', 'dec'), may hold values from -0.09375 to 0.09375
- block_order: int32 [32], P('groups'), parts along dimension 0, may hold values from 0 to 15, as said below
- block_docs: int32 [32], P('groups'), parts along dimension 0, may hold values from 0 to 3, never falling along the last dimension, each value on 1 to 8 neighbouring positions
- head_owner: int32 [8], P('groups'), parts along dimension 0, may hold values from 0 to 3, as said below
- prev_kv: bfloat16 [2048, 2, 4, 128], P(('groups', 'seq', 'dec')), parts along dimension 0, may hold values from -6 to 6
Outputs:
- attended: bfloat16 [2048, 2048], P(('groups', 'seq'), 'dec'), parts along dimension 0
- decode_cache: bfloat16 [2048, 2, 4, 128], P(('groups', 'seq'), None, 'dec'), parts along dimension 0
The draws below stay inside these ranges and needn't reach their ends.
There are 2 independent parts, one for each index of `groups`. The reference program is written for one: setup_inputs(seed, part) draws one part's arguments, and reference() takes and returns one part's arrays. A program takes and returns all parts, laid end to end along the dimension named above; an argument that names none is the same for every part. Nothing has to cross between parts.
Inputs may be any that keep to these rules, and one draw needn't show every extreme that they name: `block_order`: cycle slots 2i and 2i + 1 hold the blocks b and 15 - b for some b; every block stands in exactly one slot. `head_owner`: each key-value head stands in exactly one decode slot.
All inputs are finite; a program needn't handle non-finite values.
Results may differ from the reference program's by a relative error of at most 0.0035.
The reference program's roundings to bfloat16 on the way (of `normed`, `values` and `probability`) count: a program that leaves them out, or rounds other values in their place, can miss the bound.
Values may be sent and summed in bfloat16 or wider, within the bound.
A program may use at most 64 MiB of HBM per device.

```python
import math
import jax
import jax.numpy as jnp
import numpy as np
from jax import lax

D = 4096
QH = 16
KVH = 4
HD = 128
TOKENS = 1024
BLK = 64
BLOCKS = 16
N_SEQ = 8


def query_base(key):
    return 3.0 * jax.random.truncated_normal(jax.random.fold_in(key, 11), -6.0, 6.0, (D, QH * HD), jnp.float32) / math.sqrt(D)


def draw_w_query(key, part):
    bound = 9.0 / math.sqrt(D)
    return jnp.clip(query_base(key), -bound, bound).astype(jnp.bfloat16)


def draw_w_key(key, part):
    bound = 9.0 / math.sqrt(D)
    fresh = jax.random.truncated_normal(jax.random.fold_in(key, 12), -6.0, 6.0, (D, KVH, HD), jnp.float32) / math.sqrt(D)
    return jnp.clip(fresh.reshape(D, KVH * HD), -bound, bound).astype(jnp.bfloat16)


def draw_tokens(key, part):
    base = jax.random.truncated_normal(jax.random.fold_in(key, 31), -6.0, 6.0, (TOKENS, D), jnp.float32)
    return base.astype(jnp.bfloat16)


def draw_block_order(key, part):
    pairs = BLOCKS // 2
    owner = jax.random.permutation(jax.random.fold_in(key, 21), pairs)
    flipped = jax.random.randint(jax.random.fold_in(key, 22), (pairs,), 0, 2)
    lower_block = owner
    upper_block = BLOCKS - 1 - owner
    leading = jnp.where(flipped == 1, upper_block, lower_block)
    trailing = jnp.where(flipped == 1, lower_block, upper_block)
    return jnp.stack([leading, trailing], 1).reshape(BLOCKS).astype(jnp.int32)


def draw_head_owner(key, part):
    return jax.random.permutation(jax.random.fold_in(key, 41), KVH).astype(jnp.int32)


def block_scale(rng, extent, pieces, smallest, high):
    level = 1.0
    for dim, blocks in pieces:
        draws = jax.random.uniform(jax.random.fold_in(jax.random.fold_in(rng, 6), dim), (blocks,), jnp.float32, smallest / len(pieces), high / len(pieces))
        level = level * jnp.repeat(jnp.exp(draws), extent[dim] // blocks).reshape((-1,) + (1,) * (len(extent) - 1 - dim))
    return level


def length_profile(number_of, total, limit, lean):
    loads = [(1 << 20) // math.isqrt(grade ** lean) + 1 for grade in range(2, number_of + 1)]
    surplus, given = total - limit - (number_of - 1), [1] * (number_of - 1)
    while surplus > 0:
        movable = [i for i in range(number_of - 1) if given[i] < limit]
        pool, budget = sum([loads[i] for i in movable]), surplus
        for i in movable:
            extra = min(limit - given[i], max(1, budget * loads[i] // pool), surplus)
            given[i] = given[i] + extra
            surplus = surplus - extra
    return np.array([limit] + given)


def ragged_sizes(own_key, number_of, total, most, slope):
    if number_of == 2:
        one = jax.random.randint(own_key, (), max(1, total - most), min(most, total - 1) + 1)
        return jnp.stack([one, total - one])
    sizes = jnp.asarray(length_profile(number_of, total, most, slope), jnp.int32)
    couples = (number_of - 1) // 2
    source_of, sink = sizes[1:1 + 2 * couples:2], sizes[2:2 + 2 * couples:2]
    slack = jnp.minimum(source_of - 1, most - sink)
    moved = jax.random.randint(jax.random.fold_in(own_key, 1), (couples,), 0, 1 << 20) % (slack + 1)
    sizes = sizes.at[1:1 + 2 * couples:2].set(source_of - moved).at[2:2 + 2 * couples:2].set(sink + moved)
    return sizes[jax.random.permutation(jax.random.fold_in(own_key, 2), number_of)]


def bell_draw(key, extent, width, limit, shards=(), kind=jnp.bfloat16):
    values = width * jax.random.normal(key, extent, jnp.float32)
    if shards:
        values = values * block_scale(key, extent, shards, -0.22, 0.18)
    return jnp.clip(values, -limit, limit).astype(kind)


def setup_inputs(seed: int = 0, part: int = 0) -> dict:
    key_list = jax.random.split(jax.random.key(seed), 10)
    part_keys = jax.random.split(jax.random.fold_in(key_list[9], part), 10)
    tokens = draw_tokens(jax.random.fold_in(jax.random.fold_in(key_list[9], part), 71), part)
    norm_gain = jnp.clip(1.0 + 0.15 * jax.random.normal(key_list[1], (D,), jnp.float32), 0.25, 1.75)
    w_query = draw_w_query(jax.random.fold_in(key_list[9], 71), part)
    w_key = draw_w_key(jax.random.fold_in(key_list[9], 71), part)
    w_value = bell_draw(key_list[4], (D, KVH * HD), D ** -0.5, 0.09375, ((0, 8), (1, 2)))
    block_order = draw_block_order(jax.random.fold_in(jax.random.fold_in(key_list[9], part), 71), part)
    block_docs = jnp.searchsorted(jnp.cumsum(ragged_sizes(part_keys[6], N_SEQ // 2, BLOCKS, N_SEQ, 2)), jnp.arange(BLOCKS), side="right").astype(jnp.int32)
    head_owner = draw_head_owner(jax.random.fold_in(jax.random.fold_in(key_list[9], part), 71), part)
    prev_kv = bell_draw(part_keys[8], (TOKENS, 2, KVH, HD), 1.0, 6.0, ((0, 16),))
    return dict(tokens=tokens, norm_gain=norm_gain, w_query=w_query, w_key=w_key, w_value=w_value, block_order=block_order, block_docs=block_docs, head_owner=head_owner, prev_kv=prev_kv)


def rotate(values, positions):
    half_width = values.shape[-1] // 2
    frequency = 500000.0 ** (-jnp.arange(half_width, dtype=jnp.float32) / half_width)
    angles = positions[:, None].astype(jnp.float32) * frequency[None, :]
    cosines = jnp.cos(angles)[:, None, :]
    sine_terms = jnp.sin(angles)[:, None, :]
    lower_half = values[..., :half_width]
    upper_half = values[..., half_width:]
    return jnp.concatenate([lower_half * cosines - upper_half * sine_terms, upper_half * cosines + lower_half * sine_terms], -1)

def reference(tokens, norm_gain, w_query, w_key, w_value, block_order, block_docs, head_owner, prev_kv):
    inputs = tokens.astype(jnp.float32)
    normed = (inputs * lax.rsqrt(lax.optimization_barrier(jnp.mean(inputs * inputs, -1, keepdims=True)) + 1e-05) * norm_gain).astype(jnp.bfloat16)
    row_ids = jnp.arange(TOKENS, dtype=jnp.int32)
    natural = block_order[row_ids // BLK]
    positions = natural * BLK + row_ids % BLK
    documents = block_docs[natural]
    queries = rotate(jnp.dot(normed, w_query, preferred_element_type=jnp.float32).reshape(TOKENS, QH, HD), positions).astype(jnp.bfloat16)
    key_rows = rotate(jnp.dot(normed, w_key, preferred_element_type=jnp.float32).reshape(TOKENS, KVH, HD), positions).astype(jnp.bfloat16)
    value_rows = jnp.dot(normed, w_value, preferred_element_type=jnp.float32).astype(jnp.bfloat16).reshape(TOKENS, KVH, HD)
    allowed = (positions[None, :] <= positions[:, None]) & (documents[None, :] == documents[:, None])
    group_size = QH // KVH
    scale = 1.0 / math.sqrt(HD)

    def one_head(head_index):
        query_head = queries[:, head_index]
        key_head = key_rows[:, head_index // group_size]
        value_head = value_rows[:, head_index // group_size]
        scores = jnp.dot(query_head, key_head.T, preferred_element_type=jnp.float32) * scale
        scores = jnp.where(allowed, scores, -jnp.inf)
        row_max = lax.optimization_barrier(jnp.max(scores, -1, keepdims=True))
        exponent_terms = jnp.exp(scores - row_max)
        running_sum = lax.optimization_barrier(jnp.sum(exponent_terms, -1, keepdims=True))
        probability = exponent_terms.astype(jnp.bfloat16)
        return jnp.dot(probability, value_head, preferred_element_type=jnp.float32) / running_sum
    heads_out = lax.map(one_head, jnp.arange(QH, dtype=jnp.int32))
    attended = jnp.transpose(heads_out, (1, 0, 2)).reshape(TOKENS, QH * HD).astype(jnp.bfloat16)
    decode_cache = prev_kv[:, :, head_owner, :]
    return (attended, decode_cache)
```

```python
import functools
import math

import jax
import jax.numpy as jnp
import numpy as np
from jax import lax
from jax.experimental import pallas as pl
from jax.experimental.pallas import tpu as pltpu
from jax.sharding import PartitionSpec as P

HD = 128


def rotate(values, positions):
    half_width = values.shape[-1] // 2
    frequency = 500000.0 ** (-jnp.arange(half_width, dtype=jnp.float32) / half_width)
    angles = positions[:, None].astype(jnp.float32) * frequency[None, :]
    cosines = jnp.cos(angles)[:, None, :]
    sine_terms = jnp.sin(angles)[:, None, :]
    lower_half = values[..., :half_width]
    upper_half = values[..., half_width:]
    return jnp.concatenate(
        [
            lower_half * cosines - upper_half * sine_terms,
            upper_half * cosines + lower_half * sine_terms,
        ],
        -1,
    )


def general_plan(
    tokens, norm_gain, w_query, w_key, w_value, block_order, block_docs, head_owner, prev_kv
):
    rows_dev = tokens.shape[0]
    block_rows = rows_dev // 2
    inputs = tokens.astype(jnp.float32)
    normed = (
        inputs * lax.rsqrt(jnp.mean(inputs * inputs, -1, keepdims=True) + 1e-05) * norm_gain
    ).astype(jnp.bfloat16)

    def add_piece(piece):
        return jnp.dot(normed, piece, preferred_element_type=jnp.float32)

    pieces = (
        lax.all_gather(w_query, "seq", axis=0, tiled=True),
        lax.all_gather(w_key, "seq", axis=0, tiled=True),
        lax.all_gather(w_value, "seq", axis=0, tiled=True),
    )
    query_full, key_full, value_full = tuple((add_piece(piece) for piece in pieces))
    total_rows = rows_dev * lax.axis_size("seq")
    row_ids = jnp.arange(total_rows, dtype=jnp.int32)
    natural = jnp.take(block_order, row_ids // block_rows)
    pos_all = natural * block_rows + row_ids % block_rows
    doc_all = jnp.take(block_docs, natural)
    offset = lax.axis_index("seq") * rows_dev
    my_pos = lax.dynamic_slice_in_dim(pos_all, offset, rows_dev)
    my_doc = lax.dynamic_slice_in_dim(doc_all, offset, rows_dev)
    local_kv = key_full.shape[1] // HD
    local_heads = query_full.shape[1] // HD
    group_size = local_heads // local_kv
    queries = rotate(query_full.reshape(rows_dev, local_heads, HD), my_pos).astype(jnp.bfloat16)
    query_groups = queries.reshape(rows_dev, local_kv, group_size, HD).transpose(1, 2, 0, 3)
    key_rows = (
        rotate(key_full.reshape(rows_dev, local_kv, HD), my_pos)
        .astype(jnp.bfloat16)
        .reshape(rows_dev, local_kv * HD)
    )
    value_rows = value_full.astype(jnp.bfloat16)
    scale = 1.0 / math.sqrt(HD)
    start_max = jnp.full((local_kv, group_size, rows_dev, 1), -jnp.inf, jnp.float32)
    start_sum = jnp.zeros((local_kv, group_size, rows_dev, 1), jnp.float32)
    start_weighted = jnp.zeros((local_kv, group_size, rows_dev, HD), jnp.float32)
    key_piece = lax.all_gather(key_rows, "seq", axis=0, tiled=True)
    value_piece = lax.all_gather(value_rows, "seq", axis=0, tiled=True)
    count = key_piece.shape[0]
    allowed = (pos_all[None, :] <= my_pos[:, None]) & (doc_all[None, :] == my_doc[:, None])

    def update(state):
        running_max, running_sum, weighted = state
        scores = (
            jnp.einsum(
                "ghtd,sgd->ghts",
                query_groups,
                key_piece.reshape(count, local_kv, HD),
                preferred_element_type=jnp.float32,
            )
            * scale
        )
        scores = jnp.where(allowed, scores, -jnp.inf)
        new_max = jnp.max(scores, -1, keepdims=True)
        shift_by = jnp.where(new_max == -jnp.inf, 0.0, new_max)
        weights = jnp.exp(scores - shift_by)
        rescale = jnp.exp(running_max - shift_by)
        running_sum = running_sum * rescale + jnp.sum(weights, -1, keepdims=True)
        weighted = weighted * rescale + jnp.einsum(
            "ghts,sgd->ghtd",
            weights.astype(jnp.bfloat16),
            value_piece.reshape(count, local_kv, HD),
            preferred_element_type=jnp.float32,
        )
        return (new_max, running_sum, weighted)

    final_max, final_sum, final_weighted = lax.cond(
        jnp.any(allowed), update, lambda state: state, (start_max, start_sum, start_weighted)
    )
    attended = (
        (final_weighted / final_sum)
        .transpose(2, 0, 1, 3)
        .reshape(rows_dev, local_heads * HD)
        .astype(jnp.bfloat16)
    )
    head_count = prev_kv.shape[2]
    selector = (head_owner[:, None] == jnp.arange(head_count, dtype=jnp.int32)[None, :]).astype(
        jnp.bfloat16
    )
    ordered = jnp.einsum(
        "tcjd,sj->tcsd", prev_kv, selector, preferred_element_type=jnp.float32
    ).astype(jnp.bfloat16)
    decode_cache = lax.all_to_all(ordered, "dec", split_axis=2, concat_axis=0, tiled=True)
    return (attended, decode_cache)


def attend_kernel(
    sizes,
    order_ref,
    docs_ref,
    freq_ref,
    gain_ref,
    tok_in,
    wq_in,
    wk_in,
    wv_in,
    prev_in,
    out_ref,
    prev_out,
    tok,
    wbuf,
    normed,
    qbuf,
    kvbuf,
    csbuf,
    att,
    local_sem,
    home_send,
    homeq_recv,
    homekv_recv,
    rel_send,
    rel_recv,
    own_send,
    fwd_send,
    tok_recv,
    sib_send,
    sib_recv,
    prev_sem,
    kv_send,
    kv_recv,
    att_send,
    att_recv,
):
    X, A, Y, rows, R, hpg, slots, blk, T = sizes
    Rp = R // X
    half = rows // 2
    QW = hpg * HD
    x = lax.axis_index("groups")
    q = lax.axis_index("seq")
    d = lax.axis_index("dec")
    a = q // Y
    y = q % Y
    unit = a % 2

    def dev(x_, a_, y_, d_=None):
        return {"groups": x_, "seq": a_ * Y + y_, "dec": d if d_ is None else d_}

    def remote(src, dst, ssem, rsem, device):
        return pltpu.make_async_remote_copy(
            src_ref=src,
            dst_ref=dst,
            send_sem=ssem,
            recv_sem=rsem,
            device_id=device,
            device_id_type=pl.DeviceIdType.MESH,
        )

    sibling = dev(x, a, y, 1 - d)
    barrier = pltpu.get_barrier_semaphore()
    plane = [(i, j) for i in range(X) for j in range(Y) if (i, j) != (0, 0)]
    peers = [dev((x + i) % X, a, (y + j) % Y) for i, j in plane]
    peers += [dev(x, (a + t) % A, y) for t in range(1, A)]
    mate = a + 1 - 2 * unit
    peers += [dev(x, mate, (y + j) % Y) for j in range(1, Y)]
    peers.append(sibling)
    for peer in peers:
        pl.semaphore_signal(barrier, inc=1, device_id=peer, device_id_type=pl.DeviceIdType.MESH)
    pl.semaphore_wait(barrier, len(peers))

    def w_rows(a_, y_, x_):
        return pl.ds(pl.multiple_of((a_ * Y + y_) * R + x_ * Rp, Rp), Rp)

    part = pl.ds(pl.multiple_of(x * Rp, Rp), Rp)

    def kv_source(t):
        return wv_in if t % 2 else wk_in

    def home_copies(t):
        kv_cols = pl.ds((t // 2) * HD, HD)
        return (
            remote(
                wq_in.at[part, pl.ds(t * QW, QW)],
                wbuf.at[w_rows(a, y, x), pl.ds(0, QW)],
                home_send.at[0, t],
                homeq_recv.at[a],
                dev(x, t, y),
            ),
            remote(
                kv_source(t).at[part, kv_cols],
                wbuf.at[w_rows(a, y, x), pl.ds(QW, HD)],
                home_send.at[1, t],
                homekv_recv.at[a],
                dev(x, t, y),
            ),
        )

    def local_copies(t):
        rows_all = pl.ds(pl.multiple_of(q * R, R), R)
        return (
            pltpu.make_async_copy(
                wq_in.at[:, pl.ds(t * QW, QW)],
                wbuf.at[rows_all, pl.ds(0, QW)],
                local_sem.at[0],
            ),
            pltpu.make_async_copy(
                kv_source(t).at[:, pl.ds((t // 2) * HD, HD)],
                wbuf.at[rows_all, pl.ds(QW, HD)],
                local_sem.at[1],
            ),
        )

    for t in range(A):

        @pl.when(a == t)
        def _():
            for copy in local_copies(t):
                copy.start()

        @pl.when(a != t)
        def _():
            for copy in home_copies(t):
                copy.start()

    my_half = pl.ds(pl.multiple_of(d * half, half), half)
    other_half = pl.ds(pl.multiple_of((1 - d) * half, half), half)

    def own_push(side):
        return remote(
            tok_in.at[my_half],
            tok.at[a, my_half],
            own_send.at[side],
            tok_recv.at[a],
            dev(x, a + 1 - 2 * side, y),
        )

    @pl.when(a + 1 < A)
    def _():
        own_push(0).start()

    @pl.when(a >= 1)
    def _():
        own_push(1).start()

    own_tok = pltpu.make_async_copy(tok_in, tok.at[a], local_sem.at[2])
    own_tok.start()
    prev_copy = remote(prev_in, prev_out, prev_sem.at[0], prev_sem.at[1], sibling)
    prev_copy.start()

    def relay(t, index, i, j):
        src = wbuf.at[w_rows(t, y, x)]
        return remote(
            src,
            src,
            rel_send.at[t, index],
            rel_recv.at[t, y, x],
            dev((x + i) % X, a, (y + j) % Y),
        )

    for t in range(A):

        @pl.when(a == t)
        def _():
            for copy in local_copies(t):
                copy.wait()
            for index, (i, j) in enumerate(plane):
                if j:
                    relay(t, index, i, j).start()

    lane = lax.broadcasted_iota(jnp.int32, (rows, HD), 1)
    row_id = lax.broadcasted_iota(jnp.int32, (rows, 1), 0)

    def row_values(c, table):
        value = jnp.zeros((rows, 1), jnp.int32)
        for i in range(slots):
            entry = table(order_ref[(c * Y + y) * slots + i])
            value = jnp.where(row_id // blk == i, entry, value)
        return value

    def row_positions(c):
        return row_values(c, lambda n: n) * blk + row_id % blk

    for o in range(1, A):
        t = (a + o) % A
        src = wbuf.at[w_rows(t, y, x)]
        remote(
            wq_in.at[part, pl.ds(0, QW)],
            wbuf.at[w_rows(t, y, x), pl.ds(0, QW)],
            home_send.at[0, 0],
            homeq_recv.at[t],
            sibling,
        ).wait_recv()
        remote(
            wk_in.at[part, pl.ds(0, HD)],
            wbuf.at[w_rows(t, y, x), pl.ds(QW, HD)],
            home_send.at[1, 0],
            homekv_recv.at[t],
            sibling,
        ).wait_recv()
        for index, (i, j) in enumerate(plane):
            relay(t, index, i, j).start()

    def forward(c, to):
        return remote(
            tok.at[c, my_half],
            tok.at[c, my_half],
            fwd_send.at[c],
            tok_recv.at[c],
            dev(x, to, y),
        )

    def share(c):
        return remote(
            tok.at[c, my_half], tok.at[c, my_half], sib_send.at[c], sib_recv.at[c], sibling
        )

    def token_step(s):
        @pl.when(a >= s)
        def _():
            c = a - s
            forward(c, a).wait_recv()

            @pl.when(a + 1 < A)
            def _():
                forward(c, a + 1).start()

            share(c).start()

        @pl.when(a + s < A)
        def _():
            c = a + s
            forward(c, a).wait_recv()

            @pl.when(a >= 1)
            def _():
                forward(c, a - 1).start()

            share(c).start()

    def pick(s):
        value, bit = 0, 1
        while bit < A:
            value = value + bit * ((a // bit + s // bit) % 2)
            bit *= 2
        return value

    def kv_peer(dy, da):
        return dev(x, a - unit + (unit + da) % 2, (y + dy) % Y)

    kv_plan = [(dy, da) for dy in range(Y) for da in range(2) if (dy, da) != (0, 0)]

    def kv_push(s, c, index, dy, da):
        src = kvbuf.at[unit, c * Y + y]
        return remote(src, src, kv_send.at[s, index], kv_recv.at[unit, c, y], kv_peer(dy, da))

    def normalize(s):
        c = pick(s)
        if s == 0:
            own_tok.wait()
        else:
            other = tok.at[c, other_half]
            remote(other, other, sib_send.at[c], sib_recv.at[c], sibling).wait_recv()

        def block(i, carry):
            span = pl.ds(pl.multiple_of(i * 16, 16), 16)
            inputs = tok[c, span].astype(jnp.float32)
            mean = jnp.mean(inputs * inputs, -1, keepdims=True)
            normed[c, span] = (inputs * lax.rsqrt(mean + 1e-05) * gain_ref[...]).astype(
                jnp.bfloat16
            )
            return carry

        lax.fori_loop(0, rows // 16, block, 0, unroll=2)

    def project(s, carry):
        c = pick(s)
        cosine = csbuf[0, c]
        sine = csbuf[1, c]

        def turn(v):
            return v * cosine + pltpu.roll(v, HD // 2, 1) * sine

        raw = jnp.dot(normed[c], wbuf[:, QW:], preferred_element_type=jnp.float32)
        kvbuf[unit, c * Y + y] = jnp.where(unit == 0, turn(raw), raw).astype(jnp.bfloat16)
        product = jnp.dot(normed[c], wbuf[:, :QW], preferred_element_type=jnp.float32)
        for index, (dy, da) in enumerate(kv_plan):
            kv_push(s, c, index, dy, da).start()
        for h in range(hpg):
            qbuf[c, :, h * HD : (h + 1) * HD] = turn(product[:, h * HD : (h + 1) * HD]).astype(
                jnp.bfloat16
            )
        return carry

    step_angle = (row_id % blk).astype(jnp.float32) * freq_ref[...]
    step_cos = jnp.cos(step_angle)
    step_sin = jnp.sin(step_angle)
    sign = jnp.where(lane < HD // 2, -1.0, 1.0)
    entry_id = lax.broadcasted_iota(jnp.int32, (A * slots, 1), 0)
    entries = jnp.zeros((A * slots, 1), jnp.int32)
    for c in range(A):
        for i in range(slots):
            entries = jnp.where(
                entry_id == c * slots + i, order_ref[(c * Y + y) * slots + i], entries
            )
    base_angle = (entries * blk).astype(jnp.float32) * freq_ref[...]
    base_cos = jnp.cos(base_angle)
    base_sin = jnp.sin(base_angle)
    for c in range(A):
        row_cos = jnp.broadcast_to(base_cos[c * slots : c * slots + 1], (rows, HD))
        row_sin = jnp.broadcast_to(base_sin[c * slots : c * slots + 1], (rows, HD))
        for i in range(1, slots):
            k = c * slots + i
            row_cos = jnp.where(row_id // blk == i, base_cos[k : k + 1], row_cos)
            row_sin = jnp.where(row_id // blk == i, base_sin[k : k + 1], row_sin)
        csbuf[0, c] = row_cos * step_cos - row_sin * step_sin
        csbuf[1, c] = (row_sin * step_cos + row_cos * step_sin) * sign

    normalize(0)
    for s in range(1, A - 1):
        token_step(s)
        normalize(s)
    for o in range(A):
        t = (a + o) % A
        for i, j in plane:
            if o or j:
                src = wbuf.at[w_rows(t, (y + j) % Y, (x + i) % X)]
                remote(
                    src,
                    src,
                    rel_send.at[0, 0],
                    rel_recv.at[t, (y + j) % Y, (x + i) % X],
                    sibling,
                ).wait_recv()

    lax.fori_loop(0, A - 1, project, 0)
    token_step(A - 1)
    normalize(A - 1)
    project(A - 1, 0)

    for s in range(A):
        c = pick(s)
        for dy, da in kv_plan:
            u = (unit + da) % 2
            dst = kvbuf.at[u, c * Y + (y + dy) % Y]
            remote(
                dst, dst, kv_send.at[0, 0], kv_recv.at[u, c, (y + dy) % Y], sibling
            ).wait_recv()

    key_id = lax.broadcasted_iota(jnp.int32, (1, T), 1)
    key_pos = jnp.zeros((1, T), jnp.int32)
    key_doc = jnp.zeros((1, T), jnp.int32)
    for i in range(T // blk):
        here = key_id // blk == i
        natural = order_ref[i]
        key_pos = jnp.where(here, natural * blk, key_pos)
        key_doc = jnp.where(here, docs_ref[natural], key_doc)
    key_pos = key_pos + key_id % blk
    scale = 1.0 / math.sqrt(HD)
    out_cols = pl.ds(pl.multiple_of(a * QW, QW), QW)

    def att_push(s, c):
        return remote(
            att.at[c], out_ref.at[:, out_cols], att_send.at[s], att_recv.at[a], dev(x, c, y)
        )

    def attend(s, carry):
        c = pick(A - 1 - s)
        allowed = (key_pos <= row_positions(c)) & (
            key_doc == row_values(c, lambda n: docs_ref[n])
        )
        keys = kvbuf[0].reshape(T, HD)
        values = kvbuf[1].reshape(T, HD)
        for h in range(hpg):
            scores = (
                lax.dot_general(
                    qbuf[c, :, h * HD : (h + 1) * HD],
                    keys,
                    (((1,), (1,)), ((), ())),
                    preferred_element_type=jnp.float32,
                )
                * scale
            )
            scores = jnp.where(allowed, scores, -jnp.inf)
            weights = jnp.exp(scores - jnp.max(scores, -1, keepdims=True))
            total = jnp.sum(weights, -1, keepdims=True)
            weighted = jnp.dot(
                weights.astype(jnp.bfloat16), values, preferred_element_type=jnp.float32
            )
            att[c, :, h * HD : (h + 1) * HD] = (weighted / total).astype(jnp.bfloat16)

        @pl.when(s < A - 1)
        def _():
            att_push(s, c).start()

        return carry

    lax.fori_loop(0, A, attend, 0)
    own_out = pltpu.make_async_copy(att.at[a], out_ref.at[:, out_cols], local_sem.at[3])
    own_out.start()

    for t in range(A):

        @pl.when(a != t)
        def _():
            for copy in home_copies(t):
                copy.wait_send()
            for index, (i, j) in enumerate(plane):
                relay(t, index, i, j).wait_send()

        @pl.when(a == t)
        def _():
            for index, (i, j) in enumerate(plane):
                if j:
                    relay(t, index, i, j).wait_send()

    @pl.when(a + 1 < A)
    def _():
        own_push(0).wait_send()

    @pl.when(a >= 1)
    def _():
        own_push(1).wait_send()

    for s in range(1, A):

        @pl.when(a >= s)
        def _():
            share(a - s).wait_send()

            @pl.when(a + 1 < A)
            def _():
                forward(a - s, a + 1).wait_send()

        @pl.when(a + s < A)
        def _():
            share(a + s).wait_send()

            @pl.when(a >= 1)
            def _():
                forward(a + s, a - 1).wait_send()

    for s in range(A):
        for index, (dy, da) in enumerate(kv_plan):
            kv_push(s, pick(s), index, dy, da).wait_send()
    prev_copy.wait()
    own_out.wait()
    for s in range(A - 1):
        att_push(s, pick(A - 1 - s)).wait_send()
    for o in range(1, A):
        t = (a + o) % A
        cols = pl.ds(pl.multiple_of(t * QW, QW), QW)
        remote(
            att.at[0], out_ref.at[:, cols], att_send.at[0], att_recv.at[t], sibling
        ).wait_recv()


def column_plan(
    X, tokens, norm_gain, w_query, w_key, w_value, block_order, block_docs, head_owner, prev_kv
):
    n_seq = lax.axis_size("seq")
    rows, width = tokens.shape
    R = w_query.shape[0]
    local_kv = w_key.shape[1] // HD
    local_heads = w_query.shape[1] // HD
    A = 2 * local_kv
    Y = n_seq // A
    hpg = local_heads // A
    slots = block_order.shape[0] // n_seq
    blk = rows // slots
    T = n_seq * rows
    QW = hpg * HD
    frequency = 500000.0 ** (-jnp.arange(HD // 2, dtype=jnp.float32) / (HD // 2))
    freq = jnp.concatenate([frequency, frequency])[None, :]
    sizes = (X, A, Y, rows, R, hpg, slots, blk, T)
    dma = pltpu.SemaphoreType.DMA
    smem = pl.BlockSpec(memory_space=pltpu.SMEM)
    vmem = pl.BlockSpec(memory_space=pltpu.VMEM)
    anywhere = pl.BlockSpec(memory_space=pl.ANY)
    attended, other = pl.pallas_call(
        functools.partial(attend_kernel, sizes),
        out_shape=(
            jax.ShapeDtypeStruct((rows, local_heads * HD), jnp.bfloat16),
            jax.ShapeDtypeStruct(prev_kv.shape, prev_kv.dtype),
        ),
        in_specs=[smem, smem, vmem, vmem] + [anywhere] * 5,
        out_specs=(vmem, anywhere),
        scratch_shapes=[
            pltpu.VMEM((A, rows, width), jnp.bfloat16),
            pltpu.VMEM((width, QW + HD), jnp.bfloat16),
            pltpu.VMEM((A, rows, width), jnp.bfloat16),
            pltpu.VMEM((A, rows, QW), jnp.bfloat16),
            pltpu.VMEM((2, n_seq, rows, HD), jnp.bfloat16),
            pltpu.VMEM((2, A, rows, HD), jnp.float32),
            pltpu.VMEM((A, rows, QW), jnp.bfloat16),
            dma((4,)),
            dma((2, A)),
            dma((A,)),
            dma((A,)),
            dma((A, X * Y)),
            dma((A, Y, X)),
            dma((2,)),
            dma((A,)),
            dma((A,)),
            dma((A,)),
            dma((A,)),
            dma((2,)),
            dma((A, 2 * Y)),
            dma((2, A, Y)),
            dma((A,)),
            dma((A,)),
        ],
        compiler_params=pltpu.CompilerParams(
            collective_id=0, has_side_effects=True
        ),
    )(
        block_order,
        block_docs,
        freq,
        norm_gain[None, :],
        tokens,
        w_query,
        w_key,
        w_value,
        prev_kv,
    )
    d = lax.axis_index("dec")
    head_count = prev_kv.shape[2]
    mine = head_count // 2
    owner = lax.dynamic_slice_in_dim(head_owner, d * mine, mine)
    both = jnp.concatenate(
        [jnp.where(d == 0, prev_kv, other), jnp.where(d == 0, other, prev_kv)], 0
    )
    picks = []
    for s in range(mine):
        chosen = both[:, :, 0]
        for j in range(1, head_count):
            chosen = jnp.where(owner[s] == j, both[:, :, j], chosen)
        picks.append(chosen)
    return attended, jnp.stack(picks, 2)


def quad_kernel(
    sizes,
    order_ref,
    docs_ref,
    owner_ref,
    freq_in,
    gain_in,
    tok_in,
    wq_in,
    wk_in,
    wv_in,
    prev_in,
    out_ref,
    cache_ref,
    freq,
    gain,
    tokraw,
    wbuf,
    normed,
    qbuf,
    acc,
    kvbuf,
    csbuf,
    bias,
    att,
    prev,
    picked,
    local_sem,
    init_send,
    far_send,
    pair_send,
    w_recv,
    own_send,
    pass_send,
    share_send,
    tok_recv,
    sib_recv,
    kv_send,
    kv_recv,
    att_send,
    att_recv,
    out_sem,
    cache_sem,
):
    A, rows, R, hpg, slots, blk, T, chunks, heads = sizes
    Rp = R // 2
    half = rows // 2
    step = half // chunks
    x = lax.axis_index("groups")
    q = lax.axis_index("seq")
    d = lax.axis_index("dec")
    g = q // A
    c = q % A
    u = c // 2
    y = c % 2

    def near(du, dy):
        return ((u + du) % 2) * 2 + (y + dy) % 2

    across_y, across_z, across = near(0, 1), near(1, 0), near(1, 1)

    def dev(x_, q_, d_):
        return {"groups": x_, "seq": q_, "dec": d_}

    def remote(src, dst, ssem, rsem, device):
        return pltpu.make_async_remote_copy(
            src_ref=src,
            dst_ref=dst,
            send_sem=ssem,
            recv_sem=rsem,
            device_id=device,
            device_id_type=pl.DeviceIdType.MESH,
        )

    sibling = dev(x, q, 1 - d)
    pair = dev(1 - x, q, d)
    far = dev(x, (1 - g) * A + c, d)
    quad = [dev(x, g * A + t, d) for t in (across_y, across_z, across)]

    def w_at(piece, source, part):
        return wbuf.at[piece, pl.ds(pl.multiple_of(source * R + part * Rp, Rp), Rp)]

    part_rows = pl.ds(pl.multiple_of(x * Rp, Rp), Rp)

    def start_weights(piece, t, dst, ssem, rsem, device, span):
        def go(source, column):
            src = source.at[span, pl.ds(pl.multiple_of(column, HD), HD)]
            if device is None:
                pltpu.make_async_copy(src, dst, ssem).start()
            else:
                remote(src, dst, ssem, rsem, device).start()

        if piece:
            go(wq_in, (t * hpg + piece - 1) * HD)
        else:

            @pl.when(t % 2 == 0)
            def _():
                go(wk_in, (t // 2) * HD)

            @pl.when(t % 2 == 1)
            def _():
                go(wv_in, (t // 2) * HD)

    pieces = hpg + 1
    my_half = pl.ds(pl.multiple_of(d * half, half), half)
    tok_copy = pltpu.make_async_copy(tok_in.at[my_half], tokraw, local_sem.at[pieces])
    tok_copy.start()
    gain_copy = pltpu.make_async_copy(gain_in, gain, local_sem.at[pieces + 1])
    gain_copy.start()
    freq_copy = pltpu.make_async_copy(freq_in, freq, local_sem.at[pieces + 2])
    freq_copy.start()
    prev_copy = pltpu.make_async_copy(prev_in, prev, local_sem.at[pieces + 3])
    prev_copy.start()

    def own_rows(piece):
        return wbuf.at[piece, pl.ds(pl.multiple_of(q * R, R), R)]

    for piece in range(pieces):
        start_weights(
            piece, c, own_rows(piece), local_sem.at[piece], None, None, pl.ds(0, R)
        )

    barrier = pltpu.get_barrier_semaphore()
    peers = quad + [far, pair, sibling]
    for peer in peers:
        pl.semaphore_signal(barrier, inc=1, device_id=peer, device_id_type=pl.DeviceIdType.MESH)
    pl.semaphore_wait(barrier, len(peers))

    def first_sends(piece):
        targets = [(c, far), (across, quad[2]), (across_z, quad[1]), (across_y, quad[0])]
        for i, (t, device) in enumerate(targets):
            start_weights(
                piece,
                t,
                w_at(piece, q, x),
                init_send.at[piece, i],
                w_recv.at[piece, q, x],
                device,
                part_rows,
            )

    def arrive(piece, source, part):
        ref = w_at(piece, source, part)
        remote(
            ref, ref, init_send.at[0, 0], w_recv.at[piece, source, part], sibling
        ).wait_recv()

    def relay(piece, source, sem, device):
        ref = w_at(piece, source, x)
        return remote(ref, ref, sem, w_recv.at[piece, source, x], device)

    near_sources = [g * A + t for t in (across_y, across_z, across)]
    far_sources = [(1 - g) * A + t for t in (c, across_y, across_z, across)]

    def pair_relay(piece, i):
        return relay(piece, (near_sources + far_sources)[i], pair_send.at[piece, i], pair)

    def far_relay(piece, i):
        return relay(piece, near_sources[i], far_send.at[piece, i], far)

    def near_arrivals(piece):
        for i, source in enumerate(near_sources):
            arrive(piece, source, x)
            far_relay(piece, i).start()
            pair_relay(piece, i).start()

    def far_arrivals(piece):
        for i, source in enumerate(far_sources):
            arrive(piece, source, x)
            pair_relay(piece, len(near_sources) + i).start()

    def token_rows(side, k):
        return pl.ds(pl.multiple_of(side * half + k * step, step), step)

    def token_copy(block, k, ssem, rsem, device):
        ref = normed.at[block, token_rows(d, k)]
        return remote(ref, ref, ssem, rsem, device)

    def own_copies(k):
        return (
            token_copy(c, k, own_send.at[0, k], tok_recv.at[0, k], quad[1]),
            token_copy(c, k, own_send.at[1, k], tok_recv.at[1, k], quad[0]),
            token_copy(c, k, own_send.at[2, k], sib_recv.at[3, k], sibling),
        )

    def pass_copy(k):
        return token_copy(across_z, k, pass_send.at[k], tok_recv.at[2, k], quad[0])

    token_blocks = (across_z, across_y, across)

    def share_copy(i, k):
        return token_copy(
            token_blocks[i], k, share_send.at[i, k], sib_recv.at[i, k], sibling
        )

    def token_arrival(i, k):
        ref = normed.at[token_blocks[i], token_rows(d, k)]
        remote(ref, ref, own_send.at[0, 0], tok_recv.at[i, k], sibling).wait_recv()
        if i == 0:
            pass_copy(k).start()
        share_copy(i, k).start()

    def normalize(k):
        def block(i, carry):
            span = pl.ds(pl.multiple_of(k * step + i * 16, 16), 16)
            into = pl.ds(pl.multiple_of(d * half + k * step + i * 16, 16), 16)
            inputs = tokraw[span].astype(jnp.float32)
            mean = jnp.mean(inputs * inputs, -1, keepdims=True)
            normed[c, into] = (inputs * lax.rsqrt(mean + 1e-05) * gain[...]).astype(
                jnp.bfloat16
            )
            return carry

        lax.fori_loop(0, step // 16, block, 0)

    lane = lax.broadcasted_iota(jnp.int32, (rows, HD), 1)
    row_id = lax.broadcasted_iota(jnp.int32, (rows, 1), 0)

    def make_tables():
        step_angle = (row_id % blk).astype(jnp.float32) * freq[...]
        step_cos = jnp.cos(step_angle)
        step_sin = jnp.sin(step_angle)
        sign = jnp.where(lane < HD // 2, -1.0, 1.0)
        entry_id = lax.broadcasted_iota(jnp.int32, (A * slots, 1), 0)
        entries = jnp.zeros((A * slots, 1), jnp.int32)
        for k in range(A * slots):
            entries = jnp.where(entry_id == k, order_ref[g * A * slots + k], entries)
        base_angle = (entries * blk).astype(jnp.float32) * freq[...]
        base_cos = jnp.cos(base_angle)
        base_sin = jnp.sin(base_angle)
        for b in range(A):
            row_cos = jnp.broadcast_to(base_cos[b * slots : b * slots + 1], (rows, HD))
            row_sin = jnp.broadcast_to(base_sin[b * slots : b * slots + 1], (rows, HD))
            for i in range(1, slots):
                k = b * slots + i
                row_cos = jnp.where(row_id // blk == i, base_cos[k : k + 1], row_cos)
                row_sin = jnp.where(row_id // blk == i, base_sin[k : k + 1], row_sin)
            csbuf[0, b] = row_cos * step_cos - row_sin * step_sin
            csbuf[1, b] = (row_sin * step_cos + row_cos * step_sin) * sign

    def make_bias():
        key_id = lax.broadcasted_iota(jnp.int32, (1, T), 1)
        key_pos = jnp.zeros((1, T), jnp.int32)
        key_doc = jnp.zeros((1, T), jnp.int32)
        for i in range(T // blk):
            here = key_id // blk == i
            natural = order_ref[i]
            key_pos = jnp.where(here, natural * blk, key_pos)
            key_doc = jnp.where(here, docs_ref[natural], key_doc)
        key_pos = key_pos + key_id % blk

        def block(b, carry):
            first = jnp.zeros((rows, 1), jnp.int32)
            document = jnp.zeros((rows, 1), jnp.int32)
            for i in range(slots):
                natural = order_ref[(g * A + b) * slots + i]
                here = row_id // blk == i
                first = jnp.where(here, natural * blk, first)
                document = jnp.where(here, docs_ref[natural], document)
            allowed = (key_pos <= first + row_id % blk) & (key_doc == document)
            bias[b] = jnp.where(allowed, 0.0, -jnp.inf)
            return carry

        lax.fori_loop(0, A, block, 0)

    def pick_copies():
        mine = heads // 2
        count = picked.shape[1]
        into = pl.ds(pl.multiple_of(d * count, count), count)
        return (
            pltpu.make_async_copy(picked.at[0], cache_ref.at[into], cache_sem.at[0]),
            remote(
                picked.at[1], cache_ref.at[into], cache_sem.at[1], cache_sem.at[2], sibling
            ),
        )

    def pick_heads():
        prev_copy.wait()
        mine = heads // 2
        group = HD
        taken = group // 2
        out_id = lax.broadcasted_iota(jnp.int32, (taken, group), 0)
        in_id = lax.broadcasted_iota(jnp.int32, (taken, group), 1)
        for side in range(2):
            other = d if side == 0 else 1 - d
            wanted = jnp.zeros((taken, group), jnp.int32)
            for s in range(mine):
                wanted = jnp.where(out_id % mine == s, owner_ref[other * mine + s], wanted)
            chosen = (out_id // mine == in_id // heads) & (in_id % heads == wanted)
            selector = jnp.where(chosen, 1.0, 0.0).astype(jnp.bfloat16)
            for i in range(prev.shape[0] // group):
                picked[side, i * taken : (i + 1) * taken] = jnp.dot(
                    selector,
                    prev[i * group : (i + 1) * group],
                    preferred_element_type=jnp.float32,
                ).astype(jnp.bfloat16)
        for copy in pick_copies():
            copy.start()

    def turn(v, b):
        return v * csbuf[0, b] + pltpu.roll(v, HD // 2, 1) * csbuf[1, b]

    def kv_copy(n, side, b, device):
        ref = kvbuf.at[y, side * A + b]
        return remote(ref, ref, kv_send.at[n, b], kv_recv.at[n, b], device)

    def kv_arrival(n, unit, side):
        for b in range(A):
            ref = kvbuf.at[unit, side * A + b]
            remote(ref, ref, kv_send.at[0, 0], kv_recv.at[n, b], sibling).wait_recv()
            if n == 1:
                kv_copy(2, side, b, quad[0]).start()

    def project_kv(b, carry):
        raw = jnp.dot(normed[b], wbuf[0], preferred_element_type=jnp.float32)
        kvbuf[y, g * A + b] = jnp.where(y == 0, turn(raw, b), raw).astype(jnp.bfloat16)
        kv_copy(1, g, b, far).start()
        kv_copy(0, g, b, quad[0]).start()
        return carry

    def span_of(source, part):
        return pl.ds(pl.multiple_of(source * R + part * Rp, Rp), Rp)

    def partial(piece, b, spans):
        total = None
        for span in spans:
            term = jnp.dot(
                normed[b, :, span], wbuf[piece, span], preferred_element_type=jnp.float32
            )
            total = term if total is None else total + term
        return total

    scale = 1.0 / math.sqrt(HD)

    def att_copy(h, s, b):
        cols = pl.ds(pl.multiple_of((c * hpg + h) * HD, HD), HD)
        return remote(
            att.at[h, b],
            out_ref.at[:, cols],
            att_send.at[h, s],
            att_recv.at[h, c],
            dev(x, g * A + b, d),
        )

    def own_out(h):
        cols = pl.ds(pl.multiple_of((c * hpg + h) * HD, HD), HD)
        return pltpu.make_async_copy(att.at[h, c], out_ref.at[:, cols], out_sem.at[h])

    def order(s):
        back = A - 1 - s
        return near(back // 2, back % 2)

    def attend(h, s, b, query):
        scores = (
            lax.dot_general(
                query,
                kvbuf[0].reshape(T, HD),
                (((1,), (1,)), ((), ())),
                preferred_element_type=jnp.float32,
            )
            * scale
            + bias[b]
        )
        weights = jnp.exp(scores - jnp.max(scores, -1, keepdims=True))
        total = jnp.sum(weights, -1, keepdims=True)
        weighted = jnp.dot(
            weights.astype(jnp.bfloat16),
            kvbuf[1].reshape(T, HD),
            preferred_element_type=jnp.float32,
        )
        att[h, b] = (weighted / total).astype(jnp.bfloat16)

        @pl.when(s < A - 1)
        def _():
            att_copy(h, s, b).start()

    first_sends(0)
    tok_copy.wait()
    gain_copy.wait()
    for k in range(chunks):
        normalize(k)
        for copy in own_copies(k):
            copy.start()
    freq_copy.wait()
    make_tables()
    near_arrivals(0)
    first_sends(1)
    make_bias()
    pick_heads()
    for k in range(chunks):
        token_arrival(1, k)
        token_arrival(0, k)
    far_arrivals(0)
    for k in range(chunks):
        token_arrival(2, k)
    near_arrivals(1)
    for piece in range(2, pieces):
        first_sends(piece)
    for i, block in enumerate((*token_blocks, c)):
        for k in range(chunks):
            ref = normed.at[block, token_rows(1 - d, k)]
            remote(ref, ref, own_send.at[0, 0], sib_recv.at[i, k], sibling).wait_recv()
    for piece in range(pieces):
        pltpu.make_async_copy(own_rows(piece), own_rows(piece), local_sem.at[piece]).wait()
    for source in near_sources + far_sources:
        arrive(0, source, 1 - x)
    lax.fori_loop(0, A, project_kv, 0)

    def project_all(piece):
        def project(s, carry):
            b = order(s)
            product = jnp.dot(normed[b], wbuf[piece], preferred_element_type=jnp.float32)
            qbuf[b] = turn(product, b).astype(jnp.bfloat16)
            return carry

        lax.fori_loop(0, A, project, 0)

    for h in range(hpg - 1):
        far_arrivals(1 + h)
        near_arrivals(2 + h)
        for source in near_sources + far_sources:
            arrive(1 + h, source, 1 - x)
        project_all(1 + h)
        if h == 0:
            kv_arrival(1, y, 1 - g)
            kv_arrival(0, 1 - y, g)
        if h == hpg - 2:
            far_arrivals(2 + h)
        if h == 0:
            kv_arrival(2, 1 - y, 1 - g)

        def attend_one(s, carry):
            b = order(s)
            attend(h, s, b, qbuf[b])
            return carry

        lax.fori_loop(0, A, attend_one, 0)
        own_out(h).start()

    last = hpg - 1
    early = [span_of(q, 0), span_of(q, 1)]
    early += [span_of(source, x) for source in near_sources + far_sources]

    def project_early(b, carry):
        acc[b] = partial(hpg, b, early)
        return carry

    lax.fori_loop(0, A, project_early, 0)
    for source in near_sources:
        arrive(hpg, source, 1 - x)
    middle = [span_of(source, 1 - x) for source in near_sources]

    def project_middle(b, carry):
        acc[b] += partial(hpg, b, middle)
        return carry

    lax.fori_loop(0, A, project_middle, 0)
    for source in far_sources:
        arrive(hpg, source, 1 - x)
    late = [span_of(source, 1 - x) for source in far_sources]

    def attend_last(s, carry):
        b = order(s)
        product = acc[b] + partial(hpg, b, late)
        attend(last, s, b, turn(product, b).astype(jnp.bfloat16))
        return carry

    lax.fori_loop(0, A, attend_last, 0)
    own_out(last).start()

    for piece in range(pieces):
        for i in range(A):
            ref = w_at(piece, q, x)
            remote(
                ref, ref, init_send.at[piece, i], w_recv.at[piece, q, x], far
            ).wait_send()
        for i in range(len(near_sources)):
            far_relay(piece, i).wait_send()
        for i in range(len(near_sources) + len(far_sources)):
            pair_relay(piece, i).wait_send()
    for k in range(chunks):
        for copy in own_copies(k):
            copy.wait_send()
        pass_copy(k).wait_send()
        for i in range(len(token_blocks)):
            share_copy(i, k).wait_send()
    for b in range(A):
        kv_copy(0, g, b, quad[0]).wait_send()
        kv_copy(1, g, b, far).wait_send()
        kv_copy(2, 1 - g, b, quad[0]).wait_send()
    local_pick, sent_pick = pick_copies()
    local_pick.wait()
    sent_pick.wait()
    for h in range(hpg):
        own_out(h).wait()
        for s in range(A - 1):
            att_copy(h, s, order(s)).wait_send()
        for t in (across, across_z, across_y):
            cols = pl.ds(pl.multiple_of((t * hpg + h) * HD, HD), HD)
            remote(
                att.at[h, 0], out_ref.at[:, cols], att_send.at[h, 0], att_recv.at[h, t], sibling
            ).wait_recv()


def quad_plan(
    tokens, norm_gain, w_query, w_key, w_value, block_order, block_docs, head_owner, prev_kv
):
    n_seq = lax.axis_size("seq")
    rows, width = tokens.shape
    R = w_query.shape[0]
    local_kv = w_key.shape[1] // HD
    local_heads = w_query.shape[1] // HD
    A = 2 * local_kv
    hpg = local_heads // A
    slots = block_order.shape[0] // n_seq
    blk = rows // slots
    T = n_seq * rows
    chunks = 2
    kept, planes, heads, _ = prev_kv.shape
    count = kept * planes * (heads // 2)
    frequency = 500000.0 ** (-np.arange(HD // 2, dtype=np.float64) / (HD // 2))
    freq = np.concatenate([frequency, frequency]).astype(np.float32)[None, :]
    sizes = (A, rows, R, hpg, slots, blk, T, chunks, heads)
    pieces = hpg + 1
    dma = pltpu.SemaphoreType.DMA
    smem = pl.BlockSpec(memory_space=pltpu.SMEM)
    anywhere = pl.BlockSpec(memory_space=pl.ANY)
    bf16, f32 = jnp.bfloat16, jnp.float32
    attended, cache = pl.pallas_call(
        functools.partial(quad_kernel, sizes),
        out_shape=(
            jax.ShapeDtypeStruct((rows, local_heads * HD), bf16),
            jax.ShapeDtypeStruct((2 * count, HD), prev_kv.dtype),
        ),
        in_specs=[smem] * 3 + [anywhere] * 7,
        out_specs=(anywhere, anywhere),
        scratch_shapes=[
            pltpu.VMEM((1, HD), f32),
            pltpu.VMEM((1, width), f32),
            pltpu.VMEM((rows // 2, width), bf16),
            pltpu.VMEM((pieces, width, HD), bf16),
            pltpu.VMEM((A, rows, width), bf16),
            pltpu.VMEM((A, rows, HD), bf16),
            pltpu.VMEM((A, rows, HD), f32),
            pltpu.VMEM((2, n_seq, rows, HD), bf16),
            pltpu.VMEM((2, A, rows, HD), f32),
            pltpu.VMEM((A, rows, T), f32),
            pltpu.VMEM((hpg, A, rows, HD), bf16),
            pltpu.VMEM((kept * planes * heads, HD), bf16),
            pltpu.VMEM((2, count, HD), bf16),
            dma((pieces + 4,)),
            dma((pieces, A)),
            dma((pieces, A - 1)),
            dma((pieces, n_seq - 1)),
            dma((pieces, n_seq, 2)),
            dma((3, chunks)),
            dma((chunks,)),
            dma((3, chunks)),
            dma((3, chunks)),
            dma((4, chunks)),
            dma((3, A)),
            dma((3, A)),
            dma((hpg, A)),
            dma((hpg, A)),
            dma((hpg,)),
            dma((3,)),
        ],
        compiler_params=pltpu.CompilerParams(collective_id=1, has_side_effects=True),
    )(
        block_order,
        block_docs,
        head_owner,
        freq,
        norm_gain[None, :],
        tokens,
        w_query,
        w_key,
        w_value,
        prev_kv.reshape(kept * planes * heads, HD),
    )
    return attended, cache.reshape(2 * kept, planes, heads // 2, HD)


def solution(mesh):
    in_specs = (
        P(("groups", "seq"), None),
        P(),
        P("seq", "dec"),
        P("seq", "dec"),
        P("seq", "dec"),
        P("groups"),
        P("groups"),
        P("groups"),
        P(("groups", "seq", "dec"), None, None, None),
    )
    out_specs = (P(("groups", "seq"), "dec"), P(("groups", "seq"), None, "dec", None))
    X = mesh.shape["groups"]
    n_seq = mesh.shape["seq"]

    def per_device(tokens, norm_gain, w_query, w_key, w_value, *rest):
        A = 2 * (w_key.shape[1] // HD)
        heads = w_query.shape[1] // HD
        fits = (
            mesh.shape["dec"] == 2
            and A & (A - 1) == 0
            and n_seq % A == 0
            and heads % A == 0
            and w_query.shape[0] % (16 * X) == 0
            and tokens.shape[0] % 32 == 0
        )
        squared = (
            fits
            and A == 4
            and X == 2
            and n_seq == 2 * A
            and heads >= 2 * A
            and tokens.shape[0] % 128 == 0
            and rest[-1].shape[3] == HD
            and HD % (2 * rest[-1].shape[2]) == 0
            and (rest[-1].shape[0] * rest[-1].shape[1] * rest[-1].shape[2]) % HD == 0
        )
        plan = functools.partial(column_plan, X) if fits else general_plan
        plan = quad_plan if squared else plan
        return plan(tokens, norm_gain, w_query, w_key, w_value, *rest)

    return jax.shard_map(
        per_device, mesh=mesh, in_specs=in_specs, out_specs=out_specs, check_vma=False
    )
```

```python
import functools
import math

import jax
import jax.numpy as jnp
import numpy as np
from jax import lax
from jax.experimental import pallas as pl
from jax.experimental.pallas import tpu as pltpu
from jax.sharding import PartitionSpec as P

HD = 128


def rotate(values, positions):
    half_width = values.shape[-1] // 2
    frequency = 500000.0 ** (-jnp.arange(half_width, dtype=jnp.float32) / half_width)
    angles = positions[:, None].astype(jnp.float32) * frequency[None, :]
    cosines = jnp.cos(angles)[:, None, :]
    sine_terms = jnp.sin(angles)[:, None, :]
    lower_half = values[..., :half_width]
    upper_half = values[..., half_width:]
    return jnp.concatenate(
        [
            lower_half * cosines - upper_half * sine_terms,
            upper_half * cosines + lower_half * sine_terms,
        ],
        -1,
    )


def general_plan(
    tokens, norm_gain, w_query, w_key, w_value, block_order, block_docs, head_owner, prev_kv
):
    rows_dev = tokens.shape[0]
    block_rows = rows_dev // 2
    inputs = tokens.astype(jnp.float32)
    normed = (
        inputs * lax.rsqrt(jnp.mean(inputs * inputs, -1, keepdims=True) + 1e-05) * norm_gain
    ).astype(jnp.bfloat16)

    def add_piece(piece):
        return jnp.dot(normed, piece, preferred_element_type=jnp.float32)

    pieces = (
        lax.all_gather(w_query, "seq", axis=0, tiled=True),
        lax.all_gather(w_key, "seq", axis=0, tiled=True),
        lax.all_gather(w_value, "seq", axis=0, tiled=True),
    )
    query_full, key_full, value_full = tuple((add_piece(piece) for piece in pieces))
    total_rows = rows_dev * lax.axis_size("seq")
    row_ids = jnp.arange(total_rows, dtype=jnp.int32)
    natural = jnp.take(block_order, row_ids // block_rows)
    pos_all = natural * block_rows + row_ids % block_rows
    doc_all = jnp.take(block_docs, natural)
    offset = lax.axis_index("seq") * rows_dev
    my_pos = lax.dynamic_slice_in_dim(pos_all, offset, rows_dev)
    my_doc = lax.dynamic_slice_in_dim(doc_all, offset, rows_dev)
    local_kv = key_full.shape[1] // HD
    local_heads = query_full.shape[1] // HD
    group_size = local_heads // local_kv
    queries = rotate(query_full.reshape(rows_dev, local_heads, HD), my_pos).astype(jnp.bfloat16)
    query_groups = queries.reshape(rows_dev, local_kv, group_size, HD).transpose(1, 2, 0, 3)
    key_rows = (
        rotate(key_full.reshape(rows_dev, local_kv, HD), my_pos)
        .astype(jnp.bfloat16)
        .reshape(rows_dev, local_kv * HD)
    )
    value_rows = value_full.astype(jnp.bfloat16)
    scale = 1.0 / math.sqrt(HD)
    start_max = jnp.full((local_kv, group_size, rows_dev, 1), -jnp.inf, jnp.float32)
    start_sum = jnp.zeros((local_kv, group_size, rows_dev, 1), jnp.float32)
    start_weighted = jnp.zeros((local_kv, group_size, rows_dev, HD), jnp.float32)
    key_piece = lax.all_gather(key_rows, "seq", axis=0, tiled=True)
    value_piece = lax.all_gather(value_rows, "seq", axis=0, tiled=True)
    count = key_piece.shape[0]
    allowed = (pos_all[None, :] <= my_pos[:, None]) & (doc_all[None, :] == my_doc[:, None])

    def update(state):
        running_max, running_sum, weighted = state
        scores = (
            jnp.einsum(
                "ghtd,sgd->ghts",
                query_groups,
                key_piece.reshape(count, local_kv, HD),
                preferred_element_type=jnp.float32,
            )
            * scale
        )
        scores = jnp.where(allowed, scores, -jnp.inf)
        new_max = jnp.max(scores, -1, keepdims=True)
        shift_by = jnp.where(new_max == -jnp.inf, 0.0, new_max)
        weights = jnp.exp(scores - shift_by)
        rescale = jnp.exp(running_max - shift_by)
        running_sum = running_sum * rescale + jnp.sum(weights, -1, keepdims=True)
        weighted = weighted * rescale + jnp.einsum(
            "ghts,sgd->ghtd",
            weights.astype(jnp.bfloat16),
            value_piece.reshape(count, local_kv, HD),
            preferred_element_type=jnp.float32,
        )
        return (new_max, running_sum, weighted)

    final_max, final_sum, final_weighted = lax.cond(
        jnp.any(allowed), update, lambda state: state, (start_max, start_sum, start_weighted)
    )
    attended = (
        (final_weighted / final_sum)
        .transpose(2, 0, 1, 3)
        .reshape(rows_dev, local_heads * HD)
        .astype(jnp.bfloat16)
    )
    head_count = prev_kv.shape[2]
    selector = (head_owner[:, None] == jnp.arange(head_count, dtype=jnp.int32)[None, :]).astype(
        jnp.bfloat16
    )
    ordered = jnp.einsum(
        "tcjd,sj->tcsd", prev_kv, selector, preferred_element_type=jnp.float32
    ).astype(jnp.bfloat16)
    decode_cache = lax.all_to_all(ordered, "dec", split_axis=2, concat_axis=0, tiled=True)
    return (attended, decode_cache)


def attend_kernel(
    sizes,
    order_ref,
    docs_ref,
    freq_ref,
    gain_ref,
    tok_in,
    wq_in,
    wk_in,
    wv_in,
    prev_in,
    out_ref,
    prev_out,
    tok,
    wbuf,
    normed,
    qbuf,
    kvbuf,
    csbuf,
    att,
    local_sem,
    home_send,
    homeq_recv,
    homekv_recv,
    rel_send,
    rel_recv,
    own_send,
    fwd_send,
    tok_recv,
    sib_send,
    sib_recv,
    prev_sem,
    kv_send,
    kv_recv,
    att_send,
    att_recv,
):
    X, A, Y, rows, R, hpg, slots, blk, T = sizes
    Rp = R // X
    half = rows // 2
    QW = hpg * HD
    x = lax.axis_index("groups")
    q = lax.axis_index("seq")
    d = lax.axis_index("dec")
    a = q // Y
    y = q % Y
    unit = a % 2

    def dev(x_, a_, y_, d_=None):
        return {"groups": x_, "seq": a_ * Y + y_, "dec": d if d_ is None else d_}

    def remote(src, dst, ssem, rsem, device):
        return pltpu.make_async_remote_copy(
            src_ref=src,
            dst_ref=dst,
            send_sem=ssem,
            recv_sem=rsem,
            device_id=device,
            device_id_type=pl.DeviceIdType.MESH,
        )

    sibling = dev(x, a, y, 1 - d)
    barrier = pltpu.get_barrier_semaphore()
    plane = [(i, j) for i in range(X) for j in range(Y) if (i, j) != (0, 0)]
    peers = [dev((x + i) % X, a, (y + j) % Y) for i, j in plane]
    peers += [dev(x, (a + t) % A, y) for t in range(1, A)]
    mate = a + 1 - 2 * unit
    peers += [dev(x, mate, (y + j) % Y) for j in range(1, Y)]
    peers.append(sibling)
    for peer in peers:
        pl.semaphore_signal(barrier, inc=1, device_id=peer, device_id_type=pl.DeviceIdType.MESH)
    pl.semaphore_wait(barrier, len(peers))

    def w_rows(a_, y_, x_):
        return pl.ds(pl.multiple_of((a_ * Y + y_) * R + x_ * Rp, Rp), Rp)

    part = pl.ds(pl.multiple_of(x * Rp, Rp), Rp)

    def kv_source(t):
        return wv_in if t % 2 else wk_in

    def home_copies(t):
        kv_cols = pl.ds((t // 2) * HD, HD)
        return (
            remote(
                wq_in.at[part, pl.ds(t * QW, QW)],
                wbuf.at[w_rows(a, y, x), pl.ds(0, QW)],
                home_send.at[0, t],
                homeq_recv.at[a],
                dev(x, t, y),
            ),
            remote(
                kv_source(t).at[part, kv_cols],
                wbuf.at[w_rows(a, y, x), pl.ds(QW, HD)],
                home_send.at[1, t],
                homekv_recv.at[a],
                dev(x, t, y),
            ),
        )

    def local_copies(t):
        rows_all = pl.ds(pl.multiple_of(q * R, R), R)
        return (
            pltpu.make_async_copy(
                wq_in.at[:, pl.ds(t * QW, QW)],
                wbuf.at[rows_all, pl.ds(0, QW)],
                local_sem.at[0],
            ),
            pltpu.make_async_copy(
                kv_source(t).at[:, pl.ds((t // 2) * HD, HD)],
                wbuf.at[rows_all, pl.ds(QW, HD)],
                local_sem.at[1],
            ),
        )

    for t in range(A):

        @pl.when(a == t)
        def _():
            for copy in local_copies(t):
                copy.start()

        @pl.when(a != t)
        def _():
            for copy in home_copies(t):
                copy.start()

    my_half = pl.ds(pl.multiple_of(d * half, half), half)
    other_half = pl.ds(pl.multiple_of((1 - d) * half, half), half)

    def own_push(side):
        return remote(
            tok_in.at[my_half],
            tok.at[a, my_half],
            own_send.at[side],
            tok_recv.at[a],
            dev(x, a + 1 - 2 * side, y),
        )

    @pl.when(a + 1 < A)
    def _():
        own_push(0).start()

    @pl.when(a >= 1)
    def _():
        own_push(1).start()

    own_tok = pltpu.make_async_copy(tok_in, tok.at[a], local_sem.at[2])
    own_tok.start()
    prev_copy = remote(prev_in, prev_out, prev_sem.at[0], prev_sem.at[1], sibling)
    prev_copy.start()

    def relay(t, index, i, j):
        src = wbuf.at[w_rows(t, y, x)]
        return remote(
            src,
            src,
            rel_send.at[t, index],
            rel_recv.at[t, y, x],
            dev((x + i) % X, a, (y + j) % Y),
        )

    for t in range(A):

        @pl.when(a == t)
        def _():
            for copy in local_copies(t):
                copy.wait()
            for index, (i, j) in enumerate(plane):
                if j:
                    relay(t, index, i, j).start()

    lane = lax.broadcasted_iota(jnp.int32, (rows, HD), 1)
    row_id = lax.broadcasted_iota(jnp.int32, (rows, 1), 0)

    def row_values(c, table):
        value = jnp.zeros((rows, 1), jnp.int32)
        for i in range(slots):
            entry = table(order_ref[(c * Y + y) * slots + i])
            value = jnp.where(row_id // blk == i, entry, value)
        return value

    def row_positions(c):
        return row_values(c, lambda n: n) * blk + row_id % blk

    for o in range(1, A):
        t = (a + o) % A
        src = wbuf.at[w_rows(t, y, x)]
        remote(
            wq_in.at[part, pl.ds(0, QW)],
            wbuf.at[w_rows(t, y, x), pl.ds(0, QW)],
            home_send.at[0, 0],
            homeq_recv.at[t],
            sibling,
        ).wait_recv()
        remote(
            wk_in.at[part, pl.ds(0, HD)],
            wbuf.at[w_rows(t, y, x), pl.ds(QW, HD)],
            home_send.at[1, 0],
            homekv_recv.at[t],
            sibling,
        ).wait_recv()
        for index, (i, j) in enumerate(plane):
            relay(t, index, i, j).start()

    def forward(c, to):
        return remote(
            tok.at[c, my_half],
            tok.at[c, my_half],
            fwd_send.at[c],
            tok_recv.at[c],
            dev(x, to, y),
        )

    def share(c):
        return remote(
            tok.at[c, my_half], tok.at[c, my_half], sib_send.at[c], sib_recv.at[c], sibling
        )

    def token_step(s):
        @pl.when(a >= s)
        def _():
            c = a - s
            forward(c, a).wait_recv()

            @pl.when(a + 1 < A)
            def _():
                forward(c, a + 1).start()

            share(c).start()

        @pl.when(a + s < A)
        def _():
            c = a + s
            forward(c, a).wait_recv()

            @pl.when(a >= 1)
            def _():
                forward(c, a - 1).start()

            share(c).start()

    def pick(s):
        value, bit = 0, 1
        while bit < A:
            value = value + bit * ((a // bit + s // bit) % 2)
            bit *= 2
        return value

    def kv_peer(dy, da):
        return dev(x, a - unit + (unit + da) % 2, (y + dy) % Y)

    kv_plan = [(dy, da) for dy in range(Y) for da in range(2) if (dy, da) != (0, 0)]

    def kv_push(s, c, index, dy, da):
        src = kvbuf.at[unit, c * Y + y]
        return remote(src, src, kv_send.at[s, index], kv_recv.at[unit, c, y], kv_peer(dy, da))

    def normalize(s):
        c = pick(s)
        if s == 0:
            own_tok.wait()
        else:
            other = tok.at[c, other_half]
            remote(other, other, sib_send.at[c], sib_recv.at[c], sibling).wait_recv()

        def block(i, carry):
            span = pl.ds(pl.multiple_of(i * 16, 16), 16)
            inputs = tok[c, span].astype(jnp.float32)
            mean = jnp.mean(inputs * inputs, -1, keepdims=True)
            normed[c, span] = (inputs * lax.rsqrt(mean + 1e-05) * gain_ref[...]).astype(
                jnp.bfloat16
            )
            return carry

        lax.fori_loop(0, rows // 16, block, 0, unroll=2)

    def project(s, carry):
        c = pick(s)
        cosine = csbuf[0, c]
        sine = csbuf[1, c]

        def turn(v):
            return v * cosine + pltpu.roll(v, HD // 2, 1) * sine

        raw = jnp.dot(normed[c], wbuf[:, QW:], preferred_element_type=jnp.float32)
        kvbuf[unit, c * Y + y] = jnp.where(unit == 0, turn(raw), raw).astype(jnp.bfloat16)
        product = jnp.dot(normed[c], wbuf[:, :QW], preferred_element_type=jnp.float32)
        for index, (dy, da) in enumerate(kv_plan):
            kv_push(s, c, index, dy, da).start()
        for h in range(hpg):
            qbuf[c, :, h * HD : (h + 1) * HD] = turn(product[:, h * HD : (h + 1) * HD]).astype(
                jnp.bfloat16
            )
        return carry

    step_angle = (row_id % blk).astype(jnp.float32) * freq_ref[...]
    step_cos = jnp.cos(step_angle)
    step_sin = jnp.sin(step_angle)
    sign = jnp.where(lane < HD // 2, -1.0, 1.0)
    entry_id = lax.broadcasted_iota(jnp.int32, (A * slots, 1), 0)
    entries = jnp.zeros((A * slots, 1), jnp.int32)
    for c in range(A):
        for i in range(slots):
            entries = jnp.where(
                entry_id == c * slots + i, order_ref[(c * Y + y) * slots + i], entries
            )
    base_angle = (entries * blk).astype(jnp.float32) * freq_ref[...]
    base_cos = jnp.cos(base_angle)
    base_sin = jnp.sin(base_angle)
    for c in range(A):
        row_cos = jnp.broadcast_to(base_cos[c * slots : c * slots + 1], (rows, HD))
        row_sin = jnp.broadcast_to(base_sin[c * slots : c * slots + 1], (rows, HD))
        for i in range(1, slots):
            k = c * slots + i
            row_cos = jnp.where(row_id // blk == i, base_cos[k : k + 1], row_cos)
            row_sin = jnp.where(row_id // blk == i, base_sin[k : k + 1], row_sin)
        csbuf[0, c] = row_cos * step_cos - row_sin * step_sin
        csbuf[1, c] = (row_sin * step_cos + row_cos * step_sin) * sign

    normalize(0)
    for s in range(1, A - 1):
        token_step(s)
        normalize(s)
    for o in range(A):
        t = (a + o) % A
        for i, j in plane:
            if o or j:
                src = wbuf.at[w_rows(t, (y + j) % Y, (x + i) % X)]
                remote(
                    src,
                    src,
                    rel_send.at[0, 0],
                    rel_recv.at[t, (y + j) % Y, (x + i) % X],
                    sibling,
                ).wait_recv()

    lax.fori_loop(0, A - 1, project, 0)
    token_step(A - 1)
    normalize(A - 1)
    project(A - 1, 0)

    for s in range(A):
        c = pick(s)
        for dy, da in kv_plan:
            u = (unit + da) % 2
            dst = kvbuf.at[u, c * Y + (y + dy) % Y]
            remote(
                dst, dst, kv_send.at[0, 0], kv_recv.at[u, c, (y + dy) % Y], sibling
            ).wait_recv()

    key_id = lax.broadcasted_iota(jnp.int32, (1, T), 1)
    key_pos = jnp.zeros((1, T), jnp.int32)
    key_doc = jnp.zeros((1, T), jnp.int32)
    for i in range(T // blk):
        here = key_id // blk == i
        natural = order_ref[i]
        key_pos = jnp.where(here, natural * blk, key_pos)
        key_doc = jnp.where(here, docs_ref[natural], key_doc)
    key_pos = key_pos + key_id % blk
    scale = 1.0 / math.sqrt(HD)
    out_cols = pl.ds(pl.multiple_of(a * QW, QW), QW)

    def att_push(s, c):
        return remote(
            att.at[c], out_ref.at[:, out_cols], att_send.at[s], att_recv.at[a], dev(x, c, y)
        )

    def attend(s, carry):
        c = pick(A - 1 - s)
        allowed = (key_pos <= row_positions(c)) & (
            key_doc == row_values(c, lambda n: docs_ref[n])
        )
        keys = kvbuf[0].reshape(T, HD)
        values = kvbuf[1].reshape(T, HD)
        for h in range(hpg):
            scores = (
                lax.dot_general(
                    qbuf[c, :, h * HD : (h + 1) * HD],
                    keys,
                    (((1,), (1,)), ((), ())),
                    preferred_element_type=jnp.float32,
                )
                * scale
            )
            scores = jnp.where(allowed, scores, -jnp.inf)
            weights = jnp.exp(scores - jnp.max(scores, -1, keepdims=True))
            total = jnp.sum(weights, -1, keepdims=True)
            weighted = jnp.dot(
                weights.astype(jnp.bfloat16), values, preferred_element_type=jnp.float32
            )
            att[c, :, h * HD : (h + 1) * HD] = (weighted / total).astype(jnp.bfloat16)

        @pl.when(s < A - 1)
        def _():
            att_push(s, c).start()

        return carry

    lax.fori_loop(0, A, attend, 0)
    own_out = pltpu.make_async_copy(att.at[a], out_ref.at[:, out_cols], local_sem.at[3])
    own_out.start()

    for t in range(A):

        @pl.when(a != t)
        def _():
            for copy in home_copies(t):
                copy.wait_send()
            for index, (i, j) in enumerate(plane):
                relay(t, index, i, j).wait_send()

        @pl.when(a == t)
        def _():
            for index, (i, j) in enumerate(plane):
                if j:
                    relay(t, index, i, j).wait_send()

    @pl.when(a + 1 < A)
    def _():
        own_push(0).wait_send()

    @pl.when(a >= 1)
    def _():
        own_push(1).wait_send()

    for s in range(1, A):

        @pl.when(a >= s)
        def _():
            share(a - s).wait_send()

            @pl.when(a + 1 < A)
            def _():
                forward(a - s, a + 1).wait_send()

        @pl.when(a + s < A)
        def _():
            share(a + s).wait_send()

            @pl.when(a >= 1)
            def _():
                forward(a + s, a - 1).wait_send()

    for s in range(A):
        for index, (dy, da) in enumerate(kv_plan):
            kv_push(s, pick(s), index, dy, da).wait_send()
    prev_copy.wait()
    own_out.wait()
    for s in range(A - 1):
        att_push(s, pick(A - 1 - s)).wait_send()
    for o in range(1, A):
        t = (a + o) % A
        cols = pl.ds(pl.multiple_of(t * QW, QW), QW)
        remote(
            att.at[0], out_ref.at[:, cols], att_send.at[0], att_recv.at[t], sibling
        ).wait_recv()


def column_plan(
    X, tokens, norm_gain, w_query, w_key, w_value, block_order, block_docs, head_owner, prev_kv
):
    n_seq = lax.axis_size("seq")
    rows, width = tokens.shape
    R = w_query.shape[0]
    local_kv = w_key.shape[1] // HD
    local_heads = w_query.shape[1] // HD
    A = 2 * local_kv
    Y = n_seq // A
    hpg = local_heads // A
    slots = block_order.shape[0] // n_seq
    blk = rows // slots
    T = n_seq * rows
    QW = hpg * HD
    frequency = 500000.0 ** (-jnp.arange(HD // 2, dtype=jnp.float32) / (HD // 2))
    freq = jnp.concatenate([frequency, frequency])[None, :]
    sizes = (X, A, Y, rows, R, hpg, slots, blk, T)
    dma = pltpu.SemaphoreType.DMA
    smem = pl.BlockSpec(memory_space=pltpu.SMEM)
    vmem = pl.BlockSpec(memory_space=pltpu.VMEM)
    anywhere = pl.BlockSpec(memory_space=pl.ANY)
    attended, other = pl.pallas_call(
        functools.partial(attend_kernel, sizes),
        out_shape=(
            jax.ShapeDtypeStruct((rows, local_heads * HD), jnp.bfloat16),
            jax.ShapeDtypeStruct(prev_kv.shape, prev_kv.dtype),
        ),
        in_specs=[smem, smem, vmem, vmem] + [anywhere] * 5,
        out_specs=(vmem, anywhere),
        scratch_shapes=[
            pltpu.VMEM((A, rows, width), jnp.bfloat16),
            pltpu.VMEM((width, QW + HD), jnp.bfloat16),
            pltpu.VMEM((A, rows, width), jnp.bfloat16),
            pltpu.VMEM((A, rows, QW), jnp.bfloat16),
            pltpu.VMEM((2, n_seq, rows, HD), jnp.bfloat16),
            pltpu.VMEM((2, A, rows, HD), jnp.float32),
            pltpu.VMEM((A, rows, QW), jnp.bfloat16),
            dma((4,)),
            dma((2, A)),
            dma((A,)),
            dma((A,)),
            dma((A, X * Y)),
            dma((A, Y, X)),
            dma((2,)),
            dma((A,)),
            dma((A,)),
            dma((A,)),
            dma((A,)),
            dma((2,)),
            dma((A, 2 * Y)),
            dma((2, A, Y)),
            dma((A,)),
            dma((A,)),
        ],
        compiler_params=pltpu.CompilerParams(
            collective_id=0, has_side_effects=True
        ),
    )(
        block_order,
        block_docs,
        freq,
        norm_gain[None, :],
        tokens,
        w_query,
        w_key,
        w_value,
        prev_kv,
    )
    d = lax.axis_index("dec")
    head_count = prev_kv.shape[2]
    mine = head_count // 2
    owner = lax.dynamic_slice_in_dim(head_owner, d * mine, mine)
    both = jnp.concatenate(
        [jnp.where(d == 0, prev_kv, other), jnp.where(d == 0, other, prev_kv)], 0
    )
    picks = []
    for s in range(mine):
        chosen = both[:, :, 0]
        for j in range(1, head_count):
            chosen = jnp.where(owner[s] == j, both[:, :, j], chosen)
        picks.append(chosen)
    return attended, jnp.stack(picks, 2)


PLAN = (
    ("first", 0, 2), ("first", 1, 2), ("first", 2, 3), ("first", 0, 3), ("first", 1, 3),
    ("first", 1, 0), ("first", 1, 1), ("first", 0, 1), ("near", 2, 0), ("near", 0, 1),
    ("far", 1, 0), ("spare", 0), ("spare", 1), ("own", 1), ("own", 0), ("near", 0, 0),
    ("far", 2, 1), ("first", 0, 0), ("near", 1, 0), ("near", 0, 2), ("near", 1, 1),
    ("far", 0, 2), ("tok", 0, 1), ("tok", 0, 0), ("first", 2, 2), ("tok", 1, 0),
    ("far", 0, 0), ("first", 2, 0), ("far", 0, 1), ("far", 0, 3), ("tok", 2, 1),
    ("near", 1, 2), ("near", 2, 1), ("far", 1, 2), ("far", 1, 1), ("tok", 1, 1),
    ("tok", 2, 0), ("first", 2, 1), ("keys",), ("far", 1, 3), ("far", 2, 0), ("kv", 0),
    ("near", 2, 2), ("far", 2, 2), ("kv", 1), ("query",), ("far", 2, 3), ("early",),
    ("kv", 2), ("head",), ("last",),
)


def quad_kernel(
    plan,
    sizes,
    order_ref,
    docs_ref,
    owner_ref,
    freq_in,
    gain_in,
    tok_in,
    wq_in,
    wk_in,
    wv_in,
    prev_in,
    out_ref,
    cache_ref,
    freq,
    gain,
    tokraw,
    wbuf,
    normed,
    qbuf,
    acc,
    kvbuf,
    csbuf,
    bias,
    att,
    prev,
    picked,
    local_sem,
    init_send,
    far_send,
    pair_send,
    w_recv,
    own_send,
    pass_send,
    share_send,
    tok_recv,
    sib_recv,
    kv_send,
    kv_recv,
    att_send,
    att_recv,
    out_sem,
    cache_sem,
):
    A, rows, R, hpg, slots, blk, T, chunks, heads = sizes
    Rp = R // 2
    half = rows // 2
    step = half // chunks
    x = lax.axis_index("groups")
    q = lax.axis_index("seq")
    d = lax.axis_index("dec")
    g = q // A
    c = q % A
    u = c // 2
    y = c % 2

    def near(du, dy):
        return ((u + du) % 2) * 2 + (y + dy) % 2

    across_y, across_z, across = near(0, 1), near(1, 0), near(1, 1)

    def dev(x_, q_, d_):
        return {"groups": x_, "seq": q_, "dec": d_}

    def remote(src, dst, ssem, rsem, device):
        return pltpu.make_async_remote_copy(
            src_ref=src,
            dst_ref=dst,
            send_sem=ssem,
            recv_sem=rsem,
            device_id=device,
            device_id_type=pl.DeviceIdType.MESH,
        )

    sibling = dev(x, q, 1 - d)
    pair = dev(1 - x, q, d)
    far = dev(x, (1 - g) * A + c, d)
    quad = [dev(x, g * A + t, d) for t in (across_y, across_z, across)]

    def w_at(piece, source, part):
        return wbuf.at[piece, pl.ds(pl.multiple_of(source * R + part * Rp, Rp), Rp)]

    part_rows = pl.ds(pl.multiple_of(x * Rp, Rp), Rp)

    def start_weights(piece, t, dst, ssem, rsem, device, span):
        def go(source, column):
            src = source.at[span, pl.ds(pl.multiple_of(column, HD), HD)]
            if device is None:
                pltpu.make_async_copy(src, dst, ssem).start()
            else:
                remote(src, dst, ssem, rsem, device).start()

        if piece:
            go(wq_in, (t * hpg + piece - 1) * HD)
        else:

            @pl.when(t % 2 == 0)
            def _():
                go(wk_in, (t // 2) * HD)

            @pl.when(t % 2 == 1)
            def _():
                go(wv_in, (t // 2) * HD)

    pieces = hpg + 1
    my_half = pl.ds(pl.multiple_of(d * half, half), half)
    tok_copy = pltpu.make_async_copy(tok_in.at[my_half], tokraw, local_sem.at[pieces])
    tok_copy.start()
    gain_copy = pltpu.make_async_copy(gain_in, gain, local_sem.at[pieces + 1])
    gain_copy.start()
    freq_copy = pltpu.make_async_copy(freq_in, freq, local_sem.at[pieces + 2])
    freq_copy.start()
    prev_copy = pltpu.make_async_copy(prev_in, prev, local_sem.at[pieces + 3])
    prev_copy.start()

    def own_rows(piece):
        return wbuf.at[piece, pl.ds(pl.multiple_of(q * R, R), R)]

    for piece in range(pieces):
        start_weights(
            piece, c, own_rows(piece), local_sem.at[piece], None, None, pl.ds(0, R)
        )

    barrier = pltpu.get_barrier_semaphore()
    peers = quad + [far, pair, sibling]
    for peer in peers:
        pl.semaphore_signal(barrier, inc=1, device_id=peer, device_id_type=pl.DeviceIdType.MESH)
    pl.semaphore_wait(barrier, len(peers))

    targets = ((c, far), (across, quad[2]), (across_z, quad[1]), (across_y, quad[0]))

    def first_send(piece, i):
        t, device = targets[i]
        start_weights(
            piece,
            t,
            w_at(piece, q, x),
            init_send.at[piece, i],
            w_recv.at[piece, q, x],
            device,
            part_rows,
        )

    def arrive(piece, source, part):
        ref = w_at(piece, source, part)
        remote(
            ref, ref, init_send.at[0, 0], w_recv.at[piece, source, part], sibling
        ).wait_recv()

    def relay(piece, source, sem, device):
        ref = w_at(piece, source, x)
        return remote(ref, ref, sem, w_recv.at[piece, source, x], device)

    near_sources = [g * A + t for t in (across_y, across_z, across)]
    far_sources = [(1 - g) * A + t for t in (c, across_y, across_z, across)]

    def pair_relay(piece, i):
        return relay(piece, (near_sources + far_sources)[i], pair_send.at[piece, i], pair)

    def far_relay(piece, i):
        return relay(piece, near_sources[i], far_send.at[piece, i], far)

    def near_arrival(piece, i):
        arrive(piece, near_sources[i], x)
        far_relay(piece, i).start()
        pair_relay(piece, i).start()

    def far_arrival(piece, i):
        arrive(piece, far_sources[i], x)
        pair_relay(piece, len(near_sources) + i).start()

    def token_rows(side, k):
        return pl.ds(pl.multiple_of(side * half + k * step, step), step)

    def token_copy(block, k, ssem, rsem, device):
        ref = normed.at[block, token_rows(d, k)]
        return remote(ref, ref, ssem, rsem, device)

    def own_copies(k):
        return (
            token_copy(c, k, own_send.at[0, k], tok_recv.at[0, k], quad[1]),
            token_copy(c, k, own_send.at[1, k], tok_recv.at[1, k], quad[0]),
            token_copy(c, k, own_send.at[2, k], sib_recv.at[3, k], sibling),
        )

    def pass_copy(k):
        return token_copy(across_z, k, pass_send.at[k], tok_recv.at[2, k], quad[0])

    token_blocks = (across_z, across_y, across)

    def share_copy(i, k):
        return token_copy(
            token_blocks[i], k, share_send.at[i, k], sib_recv.at[i, k], sibling
        )

    def token_arrival(i, k):
        ref = normed.at[token_blocks[i], token_rows(d, k)]
        remote(ref, ref, own_send.at[0, 0], tok_recv.at[i, k], sibling).wait_recv()
        if i == 0:
            pass_copy(k).start()
        share_copy(i, k).start()

    def normalize(k):
        def block(i, carry):
            span = pl.ds(pl.multiple_of(k * step + i * 16, 16), 16)
            into = pl.ds(pl.multiple_of(d * half + k * step + i * 16, 16), 16)
            inputs = tokraw[span].astype(jnp.float32)
            mean = jnp.mean(inputs * inputs, -1, keepdims=True)
            normed[c, into] = (inputs * lax.rsqrt(mean + 1e-05) * gain[...]).astype(
                jnp.bfloat16
            )
            return carry

        lax.fori_loop(0, step // 16, block, 0)

    lane = lax.broadcasted_iota(jnp.int32, (rows, HD), 1)
    row_id = lax.broadcasted_iota(jnp.int32, (rows, 1), 0)

    def make_tables():
        step_angle = (row_id % blk).astype(jnp.float32) * freq[...]
        step_cos = jnp.cos(step_angle)
        step_sin = jnp.sin(step_angle)
        sign = jnp.where(lane < HD // 2, -1.0, 1.0)
        entry_id = lax.broadcasted_iota(jnp.int32, (A * slots, 1), 0)
        entries = jnp.zeros((A * slots, 1), jnp.int32)
        for k in range(A * slots):
            entries = jnp.where(entry_id == k, order_ref[g * A * slots + k], entries)
        base_angle = (entries * blk).astype(jnp.float32) * freq[...]
        base_cos = jnp.cos(base_angle)
        base_sin = jnp.sin(base_angle)
        for b in range(A):
            row_cos = jnp.broadcast_to(base_cos[b * slots : b * slots + 1], (rows, HD))
            row_sin = jnp.broadcast_to(base_sin[b * slots : b * slots + 1], (rows, HD))
            for i in range(1, slots):
                k = b * slots + i
                row_cos = jnp.where(row_id // blk == i, base_cos[k : k + 1], row_cos)
                row_sin = jnp.where(row_id // blk == i, base_sin[k : k + 1], row_sin)
            csbuf[0, b] = row_cos * step_cos - row_sin * step_sin
            csbuf[1, b] = (row_sin * step_cos + row_cos * step_sin) * sign

    def make_bias():
        key_id = lax.broadcasted_iota(jnp.int32, (1, T), 1)
        key_pos = jnp.zeros((1, T), jnp.int32)
        key_doc = jnp.zeros((1, T), jnp.int32)
        for i in range(T // blk):
            here = key_id // blk == i
            natural = order_ref[i]
            key_pos = jnp.where(here, natural * blk, key_pos)
            key_doc = jnp.where(here, docs_ref[natural], key_doc)
        key_pos = key_pos + key_id % blk

        def block(b, carry):
            first = jnp.zeros((rows, 1), jnp.int32)
            document = jnp.zeros((rows, 1), jnp.int32)
            for i in range(slots):
                natural = order_ref[(g * A + b) * slots + i]
                here = row_id // blk == i
                first = jnp.where(here, natural * blk, first)
                document = jnp.where(here, docs_ref[natural], document)
            allowed = (key_pos <= first + row_id % blk) & (key_doc == document)
            bias[b] = jnp.where(allowed, 0.0, -jnp.inf)
            return carry

        lax.fori_loop(0, A, block, 0)

    def pick_copies():
        mine = heads // 2
        count = picked.shape[1]
        into = pl.ds(pl.multiple_of(d * count, count), count)
        return (
            pltpu.make_async_copy(picked.at[0], cache_ref.at[into], cache_sem.at[0]),
            remote(
                picked.at[1], cache_ref.at[into], cache_sem.at[1], cache_sem.at[2], sibling
            ),
        )

    def pick_heads():
        prev_copy.wait()
        mine = heads // 2
        group = HD
        taken = group // 2
        out_id = lax.broadcasted_iota(jnp.int32, (taken, group), 0)
        in_id = lax.broadcasted_iota(jnp.int32, (taken, group), 1)
        for side in range(2):
            other = d if side == 0 else 1 - d
            wanted = jnp.zeros((taken, group), jnp.int32)
            for s in range(mine):
                wanted = jnp.where(out_id % mine == s, owner_ref[other * mine + s], wanted)
            chosen = (out_id // mine == in_id // heads) & (in_id % heads == wanted)
            selector = jnp.where(chosen, 1.0, 0.0).astype(jnp.bfloat16)
            for i in range(prev.shape[0] // group):
                picked[side, i * taken : (i + 1) * taken] = jnp.dot(
                    selector,
                    prev[i * group : (i + 1) * group],
                    preferred_element_type=jnp.float32,
                ).astype(jnp.bfloat16)
        for copy in pick_copies():
            copy.start()

    def turn(v, b):
        return v * csbuf[0, b] + pltpu.roll(v, HD // 2, 1) * csbuf[1, b]

    def kv_copy(n, side, b, device):
        ref = kvbuf.at[y, side * A + b]
        return remote(ref, ref, kv_send.at[n, b], kv_recv.at[n, b], device)

    def kv_arrival(n, unit, side):
        for b in range(A):
            ref = kvbuf.at[unit, side * A + b]
            remote(ref, ref, kv_send.at[0, 0], kv_recv.at[n, b], sibling).wait_recv()
            if n == 1:
                kv_copy(2, side, b, quad[0]).start()

    def project_kv(b, carry):
        raw = jnp.dot(normed[b], wbuf[0], preferred_element_type=jnp.float32)
        kvbuf[y, g * A + b] = jnp.where(y == 0, turn(raw, b), raw).astype(jnp.bfloat16)
        kv_copy(1, g, b, far).start()
        kv_copy(0, g, b, quad[0]).start()
        return carry

    def span_of(source, part):
        return pl.ds(pl.multiple_of(source * R + part * Rp, Rp), Rp)

    def partial(piece, b, spans):
        total = None
        for span in spans:
            term = jnp.dot(
                normed[b, :, span], wbuf[piece, span], preferred_element_type=jnp.float32
            )
            total = term if total is None else total + term
        return total

    scale = 1.0 / math.sqrt(HD)

    def att_copy(h, s, b):
        cols = pl.ds(pl.multiple_of((c * hpg + h) * HD, HD), HD)
        return remote(
            att.at[h, b],
            out_ref.at[:, cols],
            att_send.at[h, s],
            att_recv.at[h, c],
            dev(x, g * A + b, d),
        )

    def own_out(h):
        cols = pl.ds(pl.multiple_of((c * hpg + h) * HD, HD), HD)
        return pltpu.make_async_copy(att.at[h, c], out_ref.at[:, cols], out_sem.at[h])

    def order(s):
        back = A - 1 - s
        return near(back // 2, back % 2)

    def attend(h, s, b, query):
        scores = (
            lax.dot_general(
                query,
                kvbuf[0].reshape(T, HD),
                (((1,), (1,)), ((), ())),
                preferred_element_type=jnp.float32,
            )
            * scale
            + bias[b]
        )
        weights = jnp.exp(scores - jnp.max(scores, -1, keepdims=True))
        total = jnp.sum(weights, -1, keepdims=True)
        weighted = jnp.dot(
            weights.astype(jnp.bfloat16),
            kvbuf[1].reshape(T, HD),
            preferred_element_type=jnp.float32,
        )
        att[h, b] = (weighted / total).astype(jnp.bfloat16)

        @pl.when(s < A - 1)
        def _():
            att_copy(h, s, b).start()

    def own_tokens(k):
        if k == plan[0]:
            tok_copy.wait()
            gain_copy.wait()
        normalize(k)
        for copy in own_copies(k):
            copy.start()

    def spare(i):
        if i:
            make_bias()
            pick_heads()
        else:
            freq_copy.wait()
            make_tables()

    def start_keys():
        for i, block in enumerate((*token_blocks, c)):
            for k in range(chunks):
                ref = normed.at[block, token_rows(1 - d, k)]
                remote(
                    ref, ref, own_send.at[0, 0], sib_recv.at[i, k], sibling
                ).wait_recv()
        for piece in range(pieces):
            pltpu.make_async_copy(
                own_rows(piece), own_rows(piece), local_sem.at[piece]
            ).wait()
        for source in near_sources + far_sources:
            arrive(0, source, 1 - x)
        lax.fori_loop(0, A, project_kv, 0)

    def project_first():
        for source in near_sources + far_sources:
            arrive(1, source, 1 - x)

        def project(s, carry):
            b = order(s)
            product = jnp.dot(normed[b], wbuf[1], preferred_element_type=jnp.float32)
            qbuf[b] = turn(product, b).astype(jnp.bfloat16)
            return carry

        lax.fori_loop(0, A, project, 0)

    def attend_first():
        def attend_one(s, carry):
            b = order(s)
            attend(0, s, b, qbuf[b])
            return carry

        lax.fori_loop(0, A, attend_one, 0)
        own_out(0).start()

    def kv_arrivals(n):
        kv_arrival(n, *((1 - y, g), (y, 1 - g), (1 - y, 1 - g))[n])

    last = hpg

    def project_early():
        early = [span_of(q, 0), span_of(q, 1)]
        early += [span_of(source, x) for source in near_sources + far_sources]

        def project(b, carry):
            acc[b] = partial(last, b, early)
            return carry

        lax.fori_loop(0, A, project, 0)

    def attend_last():
        for source in near_sources:
            arrive(last, source, 1 - x)
        middle = [span_of(source, 1 - x) for source in near_sources]

        def project(b, carry):
            acc[b] += partial(last, b, middle)
            return carry

        lax.fori_loop(0, A, project, 0)
        for source in far_sources:
            arrive(last, source, 1 - x)
        late = [span_of(source, 1 - x) for source in far_sources]

        def attend_one(s, carry):
            b = order(s)
            product = acc[b] + partial(last, b, late)
            attend(1, s, b, turn(product, b).astype(jnp.bfloat16))
            return carry

        lax.fori_loop(0, A, attend_one, 0)
        own_out(1).start()

    steps = {
        "first": first_send,
        "near": near_arrival,
        "far": far_arrival,
        "own": own_tokens,
        "tok": token_arrival,
        "spare": spare,
        "keys": start_keys,
        "kv": kv_arrivals,
        "query": project_first,
        "head": attend_first,
        "early": project_early,
        "last": attend_last,
    }
    for name, *where in plan[1]:
        steps[name](*where)

    for piece in range(pieces):
        for i in range(A):
            ref = w_at(piece, q, x)
            remote(
                ref, ref, init_send.at[piece, i], w_recv.at[piece, q, x], far
            ).wait_send()
        for i in range(len(near_sources)):
            far_relay(piece, i).wait_send()
        for i in range(len(near_sources) + len(far_sources)):
            pair_relay(piece, i).wait_send()
    for k in range(chunks):
        for copy in own_copies(k):
            copy.wait_send()
        pass_copy(k).wait_send()
        for i in range(len(token_blocks)):
            share_copy(i, k).wait_send()
    for b in range(A):
        kv_copy(0, g, b, quad[0]).wait_send()
        kv_copy(1, g, b, far).wait_send()
        kv_copy(2, 1 - g, b, quad[0]).wait_send()
    local_pick, sent_pick = pick_copies()
    local_pick.wait()
    sent_pick.wait()
    for h in range(hpg):
        own_out(h).wait()
        for s in range(A - 1):
            att_copy(h, s, order(s)).wait_send()
        for t in (across, across_z, across_y):
            cols = pl.ds(pl.multiple_of((t * hpg + h) * HD, HD), HD)
            remote(
                att.at[h, 0], out_ref.at[:, cols], att_send.at[h, 0], att_recv.at[h, t], sibling
            ).wait_recv()


def quad_plan(
    tokens, norm_gain, w_query, w_key, w_value, block_order, block_docs, head_owner, prev_kv
):
    n_seq = lax.axis_size("seq")
    rows, width = tokens.shape
    R = w_query.shape[0]
    local_kv = w_key.shape[1] // HD
    local_heads = w_query.shape[1] // HD
    A = 2 * local_kv
    hpg = local_heads // A
    slots = block_order.shape[0] // n_seq
    blk = rows // slots
    T = n_seq * rows
    owned = [where[0] for name, *where in PLAN if name == "own"]
    first_own, chunks = owned[0], len(owned)
    kept, planes, heads, _ = prev_kv.shape
    count = kept * planes * (heads // 2)
    frequency = 500000.0 ** (-np.arange(HD // 2, dtype=np.float64) / (HD // 2))
    freq = np.concatenate([frequency, frequency]).astype(np.float32)[None, :]
    sizes = (A, rows, R, hpg, slots, blk, T, chunks, heads)
    pieces = hpg + 1
    dma = pltpu.SemaphoreType.DMA
    smem = pl.BlockSpec(memory_space=pltpu.SMEM)
    anywhere = pl.BlockSpec(memory_space=pl.ANY)
    bf16, f32 = jnp.bfloat16, jnp.float32
    attended, cache = pl.pallas_call(
        functools.partial(quad_kernel, (first_own, PLAN), sizes),
        out_shape=(
            pltpu.VMEM((rows, local_heads * HD), bf16),
            pltpu.VMEM((2 * count, HD), prev_kv.dtype),
        ),
        in_specs=[smem] * 3 + [anywhere] * 7,
        out_specs=(anywhere, anywhere),
        scratch_shapes=[
            pltpu.VMEM((1, HD), f32),
            pltpu.VMEM((1, width), f32),
            pltpu.VMEM((rows // 2, width), bf16),
            pltpu.VMEM((pieces, width, HD), bf16),
            pltpu.VMEM((A, rows, width), bf16),
            pltpu.VMEM((A, rows, HD), bf16),
            pltpu.VMEM((A, rows, HD), f32),
            pltpu.VMEM((2, n_seq, rows, HD), bf16),
            pltpu.VMEM((2, A, rows, HD), f32),
            pltpu.VMEM((A, rows, T), f32),
            pltpu.VMEM((hpg, A, rows, HD), bf16),
            pltpu.VMEM((kept * planes * heads, HD), bf16),
            pltpu.VMEM((2, count, HD), bf16),
            dma((pieces + 4,)),
            dma((pieces, A)),
            dma((pieces, A - 1)),
            dma((pieces, n_seq - 1)),
            dma((pieces, n_seq, 2)),
            dma((3, chunks)),
            dma((chunks,)),
            dma((3, chunks)),
            dma((3, chunks)),
            dma((4, chunks)),
            dma((3, A)),
            dma((3, A)),
            dma((hpg, A)),
            dma((hpg, A)),
            dma((hpg,)),
            dma((3,)),
        ],
        compiler_params=pltpu.CompilerParams(collective_id=1, has_side_effects=True),
    )(
        block_order,
        block_docs,
        head_owner,
        freq,
        norm_gain[None, :],
        tokens,
        w_query,
        w_key,
        w_value,
        prev_kv.reshape(kept * planes * heads, HD),
    )
    return attended, cache.reshape(2 * kept, planes, heads // 2, HD)


def solution(mesh):
    in_specs = (
        P(("groups", "seq"), None),
        P(),
        P("seq", "dec"),
        P("seq", "dec"),
        P("seq", "dec"),
        P("groups"),
        P("groups"),
        P("groups"),
        P(("groups", "seq", "dec"), None, None, None),
    )
    out_specs = (P(("groups", "seq"), "dec"), P(("groups", "seq"), None, "dec", None))
    X = mesh.shape["groups"]
    n_seq = mesh.shape["seq"]

    def per_device(tokens, norm_gain, w_query, w_key, w_value, *rest):
        A = 2 * (w_key.shape[1] // HD)
        heads = w_query.shape[1] // HD
        fits = (
            mesh.shape["dec"] == 2
            and A & (A - 1) == 0
            and n_seq % A == 0
            and heads % A == 0
            and w_query.shape[0] % (16 * X) == 0
            and tokens.shape[0] % 32 == 0
        )
        squared = (
            fits
            and A == 4
            and X == 2
            and n_seq == 2 * A
            and heads == 2 * A
            and tokens.shape[0] % 128 == 0
            and rest[-1].shape[3] == HD
            and HD % (2 * rest[-1].shape[2]) == 0
            and (rest[-1].shape[0] * rest[-1].shape[1] * rest[-1].shape[2]) % HD == 0
        )
        plan = functools.partial(column_plan, X) if fits else general_plan
        plan = quad_plan if squared else plan
        return plan(tokens, norm_gain, w_query, w_key, w_value, *rest)

    return jax.shard_map(
        per_device, mesh=mesh, in_specs=in_specs, out_specs=out_specs, check_vma=False
    )
```

```python
import functools
import math

import jax
import jax.numpy as jnp
import numpy as np
from jax import lax
from jax.experimental import pallas as pl
from jax.experimental.pallas import tpu as pltpu
from jax.sharding import PartitionSpec as P

HD = 128


def rotate(values, positions):
    half_width = values.shape[-1] // 2
    frequency = 500000.0 ** (-jnp.arange(half_width, dtype=jnp.float32) / half_width)
    angles = positions[:, None].astype(jnp.float32) * frequency[None, :]
    cosines = jnp.cos(angles)[:, None, :]
    sine_terms = jnp.sin(angles)[:, None, :]
    lower_half = values[..., :half_width]
    upper_half = values[..., half_width:]
    return jnp.concatenate(
        [
            lower_half * cosines - upper_half * sine_terms,
            upper_half * cosines + lower_half * sine_terms,
        ],
        -1,
    )


def general_plan(
    tokens, norm_gain, w_query, w_key, w_value, block_order, block_docs, head_owner, prev_kv
):
    rows_dev = tokens.shape[0]
    block_rows = rows_dev // 2
    inputs = tokens.astype(jnp.float32)
    normed = (
        inputs * lax.rsqrt(jnp.mean(inputs * inputs, -1, keepdims=True) + 1e-05) * norm_gain
    ).astype(jnp.bfloat16)

    def add_piece(piece):
        return jnp.dot(normed, piece, preferred_element_type=jnp.float32)

    pieces = (
        lax.all_gather(w_query, "seq", axis=0, tiled=True),
        lax.all_gather(w_key, "seq", axis=0, tiled=True),
        lax.all_gather(w_value, "seq", axis=0, tiled=True),
    )
    query_full, key_full, value_full = tuple((add_piece(piece) for piece in pieces))
    total_rows = rows_dev * lax.axis_size("seq")
    row_ids = jnp.arange(total_rows, dtype=jnp.int32)
    natural = jnp.take(block_order, row_ids // block_rows)
    pos_all = natural * block_rows + row_ids % block_rows
    doc_all = jnp.take(block_docs, natural)
    offset = lax.axis_index("seq") * rows_dev
    my_pos = lax.dynamic_slice_in_dim(pos_all, offset, rows_dev)
    my_doc = lax.dynamic_slice_in_dim(doc_all, offset, rows_dev)
    local_kv = key_full.shape[1] // HD
    local_heads = query_full.shape[1] // HD
    group_size = local_heads // local_kv
    queries = rotate(query_full.reshape(rows_dev, local_heads, HD), my_pos).astype(jnp.bfloat16)
    query_groups = queries.reshape(rows_dev, local_kv, group_size, HD).transpose(1, 2, 0, 3)
    key_rows = (
        rotate(key_full.reshape(rows_dev, local_kv, HD), my_pos)
        .astype(jnp.bfloat16)
        .reshape(rows_dev, local_kv * HD)
    )
    value_rows = value_full.astype(jnp.bfloat16)
    scale = 1.0 / math.sqrt(HD)
    start_max = jnp.full((local_kv, group_size, rows_dev, 1), -jnp.inf, jnp.float32)
    start_sum = jnp.zeros((local_kv, group_size, rows_dev, 1), jnp.float32)
    start_weighted = jnp.zeros((local_kv, group_size, rows_dev, HD), jnp.float32)
    key_piece = lax.all_gather(key_rows, "seq", axis=0, tiled=True)
    value_piece = lax.all_gather(value_rows, "seq", axis=0, tiled=True)
    count = key_piece.shape[0]
    allowed = (pos_all[None, :] <= my_pos[:, None]) & (doc_all[None, :] == my_doc[:, None])

    def update(state):
        running_max, running_sum, weighted = state
        scores = (
            jnp.einsum(
                "ghtd,sgd->ghts",
                query_groups,
                key_piece.reshape(count, local_kv, HD),
                preferred_element_type=jnp.float32,
            )
            * scale
        )
        scores = jnp.where(allowed, scores, -jnp.inf)
        new_max = jnp.max(scores, -1, keepdims=True)
        shift_by = jnp.where(new_max == -jnp.inf, 0.0, new_max)
        weights = jnp.exp(scores - shift_by)
        rescale = jnp.exp(running_max - shift_by)
        running_sum = running_sum * rescale + jnp.sum(weights, -1, keepdims=True)
        weighted = weighted * rescale + jnp.einsum(
            "ghts,sgd->ghtd",
            weights.astype(jnp.bfloat16),
            value_piece.reshape(count, local_kv, HD),
            preferred_element_type=jnp.float32,
        )
        return (new_max, running_sum, weighted)

    final_max, final_sum, final_weighted = lax.cond(
        jnp.any(allowed), update, lambda state: state, (start_max, start_sum, start_weighted)
    )
    attended = (
        (final_weighted / final_sum)
        .transpose(2, 0, 1, 3)
        .reshape(rows_dev, local_heads * HD)
        .astype(jnp.bfloat16)
    )
    head_count = prev_kv.shape[2]
    selector = (head_owner[:, None] == jnp.arange(head_count, dtype=jnp.int32)[None, :]).astype(
        jnp.bfloat16
    )
    ordered = jnp.einsum(
        "tcjd,sj->tcsd", prev_kv, selector, preferred_element_type=jnp.float32
    ).astype(jnp.bfloat16)
    decode_cache = lax.all_to_all(ordered, "dec", split_axis=2, concat_axis=0, tiled=True)
    return (attended, decode_cache)


def attend_kernel(
    sizes,
    order_ref,
    docs_ref,
    freq_ref,
    gain_ref,
    tok_in,
    wq_in,
    wk_in,
    wv_in,
    prev_in,
    out_ref,
    prev_out,
    tok,
    wbuf,
    normed,
    qbuf,
    kvbuf,
    csbuf,
    att,
    local_sem,
    home_send,
    homeq_recv,
    homekv_recv,
    rel_send,
    rel_recv,
    own_send,
    fwd_send,
    tok_recv,
    sib_send,
    sib_recv,
    prev_sem,
    kv_send,
    kv_recv,
    att_send,
    att_recv,
):
    X, A, Y, rows, R, hpg, slots, blk, T = sizes
    Rp = R // X
    half = rows // 2
    QW = hpg * HD
    x = lax.axis_index("groups")
    q = lax.axis_index("seq")
    d = lax.axis_index("dec")
    a = q // Y
    y = q % Y
    unit = a % 2

    def dev(x_, a_, y_, d_=None):
        return {"groups": x_, "seq": a_ * Y + y_, "dec": d if d_ is None else d_}

    def remote(src, dst, ssem, rsem, device):
        return pltpu.make_async_remote_copy(
            src_ref=src,
            dst_ref=dst,
            send_sem=ssem,
            recv_sem=rsem,
            device_id=device,
            device_id_type=pl.DeviceIdType.MESH,
        )

    sibling = dev(x, a, y, 1 - d)
    barrier = pltpu.get_barrier_semaphore()
    plane = [(i, j) for i in range(X) for j in range(Y) if (i, j) != (0, 0)]
    peers = [dev((x + i) % X, a, (y + j) % Y) for i, j in plane]
    peers += [dev(x, (a + t) % A, y) for t in range(1, A)]
    mate = a + 1 - 2 * unit
    peers += [dev(x, mate, (y + j) % Y) for j in range(1, Y)]
    peers.append(sibling)
    for peer in peers:
        pl.semaphore_signal(barrier, inc=1, device_id=peer, device_id_type=pl.DeviceIdType.MESH)
    pl.semaphore_wait(barrier, len(peers))

    def w_rows(a_, y_, x_):
        return pl.ds(pl.multiple_of((a_ * Y + y_) * R + x_ * Rp, Rp), Rp)

    part = pl.ds(pl.multiple_of(x * Rp, Rp), Rp)

    def kv_source(t):
        return wv_in if t % 2 else wk_in

    def home_copies(t):
        kv_cols = pl.ds((t // 2) * HD, HD)
        return (
            remote(
                wq_in.at[part, pl.ds(t * QW, QW)],
                wbuf.at[w_rows(a, y, x), pl.ds(0, QW)],
                home_send.at[0, t],
                homeq_recv.at[a],
                dev(x, t, y),
            ),
            remote(
                kv_source(t).at[part, kv_cols],
                wbuf.at[w_rows(a, y, x), pl.ds(QW, HD)],
                home_send.at[1, t],
                homekv_recv.at[a],
                dev(x, t, y),
            ),
        )

    def local_copies(t):
        rows_all = pl.ds(pl.multiple_of(q * R, R), R)
        return (
            pltpu.make_async_copy(
                wq_in.at[:, pl.ds(t * QW, QW)],
                wbuf.at[rows_all, pl.ds(0, QW)],
                local_sem.at[0],
            ),
            pltpu.make_async_copy(
                kv_source(t).at[:, pl.ds((t // 2) * HD, HD)],
                wbuf.at[rows_all, pl.ds(QW, HD)],
                local_sem.at[1],
            ),
        )

    for t in range(A):

        @pl.when(a == t)
        def _():
            for copy in local_copies(t):
                copy.start()

        @pl.when(a != t)
        def _():
            for copy in home_copies(t):
                copy.start()

    my_half = pl.ds(pl.multiple_of(d * half, half), half)
    other_half = pl.ds(pl.multiple_of((1 - d) * half, half), half)

    def own_push(side):
        return remote(
            tok_in.at[my_half],
            tok.at[a, my_half],
            own_send.at[side],
            tok_recv.at[a],
            dev(x, a + 1 - 2 * side, y),
        )

    @pl.when(a + 1 < A)
    def _():
        own_push(0).start()

    @pl.when(a >= 1)
    def _():
        own_push(1).start()

    own_tok = pltpu.make_async_copy(tok_in, tok.at[a], local_sem.at[2])
    own_tok.start()
    prev_copy = remote(prev_in, prev_out, prev_sem.at[0], prev_sem.at[1], sibling)
    prev_copy.start()

    def relay(t, index, i, j):
        src = wbuf.at[w_rows(t, y, x)]
        return remote(
            src,
            src,
            rel_send.at[t, index],
            rel_recv.at[t, y, x],
            dev((x + i) % X, a, (y + j) % Y),
        )

    for t in range(A):

        @pl.when(a == t)
        def _():
            for copy in local_copies(t):
                copy.wait()
            for index, (i, j) in enumerate(plane):
                if j:
                    relay(t, index, i, j).start()

    lane = lax.broadcasted_iota(jnp.int32, (rows, HD), 1)
    row_id = lax.broadcasted_iota(jnp.int32, (rows, 1), 0)

    def row_values(c, table):
        value = jnp.zeros((rows, 1), jnp.int32)
        for i in range(slots):
            entry = table(order_ref[(c * Y + y) * slots + i])
            value = jnp.where(row_id // blk == i, entry, value)
        return value

    def row_positions(c):
        return row_values(c, lambda n: n) * blk + row_id % blk

    for o in range(1, A):
        t = (a + o) % A
        src = wbuf.at[w_rows(t, y, x)]
        remote(
            wq_in.at[part, pl.ds(0, QW)],
            wbuf.at[w_rows(t, y, x), pl.ds(0, QW)],
            home_send.at[0, 0],
            homeq_recv.at[t],
            sibling,
        ).wait_recv()
        remote(
            wk_in.at[part, pl.ds(0, HD)],
            wbuf.at[w_rows(t, y, x), pl.ds(QW, HD)],
            home_send.at[1, 0],
            homekv_recv.at[t],
            sibling,
        ).wait_recv()
        for index, (i, j) in enumerate(plane):
            relay(t, index, i, j).start()

    def forward(c, to):
        return remote(
            tok.at[c, my_half],
            tok.at[c, my_half],
            fwd_send.at[c],
            tok_recv.at[c],
            dev(x, to, y),
        )

    def share(c):
        return remote(
            tok.at[c, my_half], tok.at[c, my_half], sib_send.at[c], sib_recv.at[c], sibling
        )

    def token_step(s):
        @pl.when(a >= s)
        def _():
            c = a - s
            forward(c, a).wait_recv()

            @pl.when(a + 1 < A)
            def _():
                forward(c, a + 1).start()

            share(c).start()

        @pl.when(a + s < A)
        def _():
            c = a + s
            forward(c, a).wait_recv()

            @pl.when(a >= 1)
            def _():
                forward(c, a - 1).start()

            share(c).start()

    def pick(s):
        value, bit = 0, 1
        while bit < A:
            value = value + bit * ((a // bit + s // bit) % 2)
            bit *= 2
        return value

    def kv_peer(dy, da):
        return dev(x, a - unit + (unit + da) % 2, (y + dy) % Y)

    kv_plan = [(dy, da) for dy in range(Y) for da in range(2) if (dy, da) != (0, 0)]

    def kv_push(s, c, index, dy, da):
        src = kvbuf.at[unit, c * Y + y]
        return remote(src, src, kv_send.at[s, index], kv_recv.at[unit, c, y], kv_peer(dy, da))

    def normalize(s):
        c = pick(s)
        if s == 0:
            own_tok.wait()
        else:
            other = tok.at[c, other_half]
            remote(other, other, sib_send.at[c], sib_recv.at[c], sibling).wait_recv()

        def block(i, carry):
            span = pl.ds(pl.multiple_of(i * 16, 16), 16)
            inputs = tok[c, span].astype(jnp.float32)
            mean = jnp.mean(inputs * inputs, -1, keepdims=True)
            normed[c, span] = (inputs * lax.rsqrt(mean + 1e-05) * gain_ref[...]).astype(
                jnp.bfloat16
            )
            return carry

        lax.fori_loop(0, rows // 16, block, 0, unroll=2)

    def project(s, carry):
        c = pick(s)
        cosine = csbuf[0, c]
        sine = csbuf[1, c]

        def turn(v):
            return v * cosine + pltpu.roll(v, HD // 2, 1) * sine

        raw = jnp.dot(normed[c], wbuf[:, QW:], preferred_element_type=jnp.float32)
        kvbuf[unit, c * Y + y] = jnp.where(unit == 0, turn(raw), raw).astype(jnp.bfloat16)
        product = jnp.dot(normed[c], wbuf[:, :QW], preferred_element_type=jnp.float32)
        for index, (dy, da) in enumerate(kv_plan):
            kv_push(s, c, index, dy, da).start()
        for h in range(hpg):
            qbuf[c, :, h * HD : (h + 1) * HD] = turn(product[:, h * HD : (h + 1) * HD]).astype(
                jnp.bfloat16
            )
        return carry

    step_angle = (row_id % blk).astype(jnp.float32) * freq_ref[...]
    step_cos = jnp.cos(step_angle)
    step_sin = jnp.sin(step_angle)
    sign = jnp.where(lane < HD // 2, -1.0, 1.0)
    entry_id = lax.broadcasted_iota(jnp.int32, (A * slots, 1), 0)
    entries = jnp.zeros((A * slots, 1), jnp.int32)
    for c in range(A):
        for i in range(slots):
            entries = jnp.where(
                entry_id == c * slots + i, order_ref[(c * Y + y) * slots + i], entries
            )
    base_angle = (entries * blk).astype(jnp.float32) * freq_ref[...]
    base_cos = jnp.cos(base_angle)
    base_sin = jnp.sin(base_angle)
    for c in range(A):
        row_cos = jnp.broadcast_to(base_cos[c * slots : c * slots + 1], (rows, HD))
        row_sin = jnp.broadcast_to(base_sin[c * slots : c * slots + 1], (rows, HD))
        for i in range(1, slots):
            k = c * slots + i
            row_cos = jnp.where(row_id // blk == i, base_cos[k : k + 1], row_cos)
            row_sin = jnp.where(row_id // blk == i, base_sin[k : k + 1], row_sin)
        csbuf[0, c] = row_cos * step_cos - row_sin * step_sin
        csbuf[1, c] = (row_sin * step_cos + row_cos * step_sin) * sign

    normalize(0)
    for s in range(1, A - 1):
        token_step(s)
        normalize(s)
    for o in range(A):
        t = (a + o) % A
        for i, j in plane:
            if o or j:
                src = wbuf.at[w_rows(t, (y + j) % Y, (x + i) % X)]
                remote(
                    src,
                    src,
                    rel_send.at[0, 0],
                    rel_recv.at[t, (y + j) % Y, (x + i) % X],
                    sibling,
                ).wait_recv()

    lax.fori_loop(0, A - 1, project, 0)
    token_step(A - 1)
    normalize(A - 1)
    project(A - 1, 0)

    for s in range(A):
        c = pick(s)
        for dy, da in kv_plan:
            u = (unit + da) % 2
            dst = kvbuf.at[u, c * Y + (y + dy) % Y]
            remote(
                dst, dst, kv_send.at[0, 0], kv_recv.at[u, c, (y + dy) % Y], sibling
            ).wait_recv()

    key_id = lax.broadcasted_iota(jnp.int32, (1, T), 1)
    key_pos = jnp.zeros((1, T), jnp.int32)
    key_doc = jnp.zeros((1, T), jnp.int32)
    for i in range(T // blk):
        here = key_id // blk == i
        natural = order_ref[i]
        key_pos = jnp.where(here, natural * blk, key_pos)
        key_doc = jnp.where(here, docs_ref[natural], key_doc)
    key_pos = key_pos + key_id % blk
    scale = 1.0 / math.sqrt(HD)
    out_cols = pl.ds(pl.multiple_of(a * QW, QW), QW)

    def att_push(s, c):
        return remote(
            att.at[c], out_ref.at[:, out_cols], att_send.at[s], att_recv.at[a], dev(x, c, y)
        )

    def attend(s, carry):
        c = pick(A - 1 - s)
        allowed = (key_pos <= row_positions(c)) & (
            key_doc == row_values(c, lambda n: docs_ref[n])
        )
        keys = kvbuf[0].reshape(T, HD)
        values = kvbuf[1].reshape(T, HD)
        for h in range(hpg):
            scores = (
                lax.dot_general(
                    qbuf[c, :, h * HD : (h + 1) * HD],
                    keys,
                    (((1,), (1,)), ((), ())),
                    preferred_element_type=jnp.float32,
                )
                * scale
            )
            scores = jnp.where(allowed, scores, -jnp.inf)
            weights = jnp.exp(scores - jnp.max(scores, -1, keepdims=True))
            total = jnp.sum(weights, -1, keepdims=True)
            weighted = jnp.dot(
                weights.astype(jnp.bfloat16), values, preferred_element_type=jnp.float32
            )
            att[c, :, h * HD : (h + 1) * HD] = (weighted / total).astype(jnp.bfloat16)

        @pl.when(s < A - 1)
        def _():
            att_push(s, c).start()

        return carry

    lax.fori_loop(0, A, attend, 0)
    own_out = pltpu.make_async_copy(att.at[a], out_ref.at[:, out_cols], local_sem.at[3])
    own_out.start()

    for t in range(A):

        @pl.when(a != t)
        def _():
            for copy in home_copies(t):
                copy.wait_send()
            for index, (i, j) in enumerate(plane):
                relay(t, index, i, j).wait_send()

        @pl.when(a == t)
        def _():
            for index, (i, j) in enumerate(plane):
                if j:
                    relay(t, index, i, j).wait_send()

    @pl.when(a + 1 < A)
    def _():
        own_push(0).wait_send()

    @pl.when(a >= 1)
    def _():
        own_push(1).wait_send()

    for s in range(1, A):

        @pl.when(a >= s)
        def _():
            share(a - s).wait_send()

            @pl.when(a + 1 < A)
            def _():
                forward(a - s, a + 1).wait_send()

        @pl.when(a + s < A)
        def _():
            share(a + s).wait_send()

            @pl.when(a >= 1)
            def _():
                forward(a + s, a - 1).wait_send()

    for s in range(A):
        for index, (dy, da) in enumerate(kv_plan):
            kv_push(s, pick(s), index, dy, da).wait_send()
    prev_copy.wait()
    own_out.wait()
    for s in range(A - 1):
        att_push(s, pick(A - 1 - s)).wait_send()
    for o in range(1, A):
        t = (a + o) % A
        cols = pl.ds(pl.multiple_of(t * QW, QW), QW)
        remote(
            att.at[0], out_ref.at[:, cols], att_send.at[0], att_recv.at[t], sibling
        ).wait_recv()


def column_plan(
    X, tokens, norm_gain, w_query, w_key, w_value, block_order, block_docs, head_owner, prev_kv
):
    n_seq = lax.axis_size("seq")
    rows, width = tokens.shape
    R = w_query.shape[0]
    local_kv = w_key.shape[1] // HD
    local_heads = w_query.shape[1] // HD
    A = 2 * local_kv
    Y = n_seq // A
    hpg = local_heads // A
    slots = block_order.shape[0] // n_seq
    blk = rows // slots
    T = n_seq * rows
    QW = hpg * HD
    frequency = 500000.0 ** (-jnp.arange(HD // 2, dtype=jnp.float32) / (HD // 2))
    freq = jnp.concatenate([frequency, frequency])[None, :]
    sizes = (X, A, Y, rows, R, hpg, slots, blk, T)
    dma = pltpu.SemaphoreType.DMA
    smem = pl.BlockSpec(memory_space=pltpu.SMEM)
    vmem = pl.BlockSpec(memory_space=pltpu.VMEM)
    anywhere = pl.BlockSpec(memory_space=pl.ANY)
    attended, other = pl.pallas_call(
        functools.partial(attend_kernel, sizes),
        out_shape=(
            jax.ShapeDtypeStruct((rows, local_heads * HD), jnp.bfloat16),
            jax.ShapeDtypeStruct(prev_kv.shape, prev_kv.dtype),
        ),
        in_specs=[smem, smem, vmem, vmem] + [anywhere] * 5,
        out_specs=(vmem, anywhere),
        scratch_shapes=[
            pltpu.VMEM((A, rows, width), jnp.bfloat16),
            pltpu.VMEM((width, QW + HD), jnp.bfloat16),
            pltpu.VMEM((A, rows, width), jnp.bfloat16),
            pltpu.VMEM((A, rows, QW), jnp.bfloat16),
            pltpu.VMEM((2, n_seq, rows, HD), jnp.bfloat16),
            pltpu.VMEM((2, A, rows, HD), jnp.float32),
            pltpu.VMEM((A, rows, QW), jnp.bfloat16),
            dma((4,)),
            dma((2, A)),
            dma((A,)),
            dma((A,)),
            dma((A, X * Y)),
            dma((A, Y, X)),
            dma((2,)),
            dma((A,)),
            dma((A,)),
            dma((A,)),
            dma((A,)),
            dma((2,)),
            dma((A, 2 * Y)),
            dma((2, A, Y)),
            dma((A,)),
            dma((A,)),
        ],
        compiler_params=pltpu.CompilerParams(
            collective_id=0, has_side_effects=True
        ),
    )(
        block_order,
        block_docs,
        freq,
        norm_gain[None, :],
        tokens,
        w_query,
        w_key,
        w_value,
        prev_kv,
    )
    d = lax.axis_index("dec")
    head_count = prev_kv.shape[2]
    mine = head_count // 2
    owner = lax.dynamic_slice_in_dim(head_owner, d * mine, mine)
    both = jnp.concatenate(
        [jnp.where(d == 0, prev_kv, other), jnp.where(d == 0, other, prev_kv)], 0
    )
    picks = []
    for s in range(mine):
        chosen = both[:, :, 0]
        for j in range(1, head_count):
            chosen = jnp.where(owner[s] == j, both[:, :, j], chosen)
        picks.append(chosen)
    return attended, jnp.stack(picks, 2)


PLAN = (
    ("first", 0, 2), ("first", 1, 1), ("spare", 1), ("first", 0, 1), ("first", 1, 0),
    ("first", 2, 3), ("first", 0, 3), ("first", 1, 2), ("own", 2), ("near", 2, 0), ("own", 1),
    ("first", 0, 0), ("near", 0, 2), ("own", 0), ("near", 0, 1), ("tok", 0, 2), ("tok", 1, 2),
    ("near", 1, 2), ("own", 3), ("far", 0, 3), ("tok", 2, 2), ("first", 1, 3), ("near", 0, 0),
    ("tok", 1, 1), ("tok", 0, 1), ("near", 1, 1), ("tok", 0, 0), ("far", 0, 0), ("spare", 0),
    ("tok", 1, 0), ("first", 2, 0), ("near", 1, 0), ("first", 2, 2), ("far", 2, 1),
    ("far", 0, 2), ("far", 1, 0), ("tok", 0, 3), ("tok", 1, 3), ("far", 0, 1), ("near", 2, 1),
    ("tok", 2, 3), ("tok", 2, 1), ("far", 1, 3), ("tok", 2, 0), ("first", 2, 1),
    ("far", 1, 1), ("far", 1, 2), ("keys",), ("far", 2, 2), ("near", 2, 2), ("kv", 1),
    ("kv", 0), ("far", 2, 0), ("query",), ("far", 2, 3), ("early",), ("kv", 2), ("head",),
    ("last",),
)


def quad_kernel(
    plan,
    sizes,
    order_in,
    docs_in,
    owner_in,
    freq_in,
    gain_in,
    tok_in,
    wq_in,
    wk_in,
    wv_in,
    prev_in,
    out_ref,
    cache_ref,
    order_ref,
    docs_ref,
    owner_ref,
    stage,
    freq,
    gain,
    tokraw,
    wbuf,
    normed,
    qbuf,
    acc,
    kvbuf,
    csbuf,
    bias,
    att,
    prev,
    picked,
    local_sem,
    stage_sem,
    table_sem,
    init_send,
    far_send,
    pair_send,
    w_recv,
    pair_recv,
    own_send,
    pass_send,
    share_send,
    tok_recv,
    sib_recv,
    kv_send,
    kv_recv,
    att_send,
    att_recv,
    out_sem,
    cache_sem,
):
    A, rows, R, hpg, slots, blk, T, chunks, heads = sizes
    Rp = R // 2
    half = rows // 2
    step = half // chunks
    x = lax.axis_index("groups")
    q = lax.axis_index("seq")
    d = lax.axis_index("dec")
    g = q // A
    c = q % A
    u = c // 2
    y = c % 2

    def near(du, dy):
        return ((u + du) % 2) * 2 + (y + dy) % 2

    across_y, across_z, across = near(0, 1), near(1, 0), near(1, 1)

    def dev(x_, q_, d_):
        return {"groups": x_, "seq": q_, "dec": d_}

    def remote(src, dst, ssem, rsem, device):
        return pltpu.make_async_remote_copy(
            src_ref=src,
            dst_ref=dst,
            send_sem=ssem,
            recv_sem=rsem,
            device_id=device,
            device_id_type=pl.DeviceIdType.MESH,
        )

    sibling = dev(x, q, 1 - d)
    pair = dev(1 - x, q, d)
    far = dev(x, (1 - g) * A + c, d)
    quad = [dev(x, g * A + t, d) for t in (across_y, across_z, across)]

    def w_at(piece, source, part):
        return wbuf.at[piece, pl.ds(pl.multiple_of(source * R + part * Rp, Rp), Rp)]

    part_rows = pl.ds(pl.multiple_of(x * Rp, Rp), Rp)

    def weights(piece, t):
        if piece:
            return wq_in, (t * hpg + piece - 1) * HD
        return (wv_in if t % 2 else wk_in), (t // 2) * HD

    pieces = hpg + 1
    my_half = pl.ds(pl.multiple_of(d * half, half), half)
    tok_copy = pltpu.make_async_copy(tok_in.at[my_half], tokraw, local_sem.at[pieces])
    tok_copy.start()
    gain_copy = pltpu.make_async_copy(gain_in, gain, local_sem.at[pieces + 1])
    gain_copy.start()
    freq_copy = pltpu.make_async_copy(freq_in, freq, local_sem.at[pieces + 2])
    freq_copy.start()
    prev_copy = pltpu.make_async_copy(prev_in, prev, local_sem.at[pieces + 3])
    prev_copy.start()

    def own_rows(piece):
        return wbuf.at[piece, pl.ds(pl.multiple_of(q * R, R), R)]

    def own_copy(piece, t):
        source, column = weights(piece, t)
        return pltpu.make_async_copy(
            source.at[:, pl.ds(column, HD)], own_rows(piece), local_sem.at[piece]
        )

    def stage_copy(piece, t):
        source, column = weights(piece, t)
        return pltpu.make_async_copy(
            source.at[part_rows, pl.ds(column, HD)],
            stage.at[piece, t],
            stage_sem.at[piece],
        )

    for piece in range(pieces):
        for t in range(A):
            stage_copy(piece, t).start()

            @pl.when(c == t)
            def _():
                own_copy(piece, t).start()

    table_copies = [
        pltpu.make_async_copy(source, into, table_sem.at[i])
        for i, (source, into) in enumerate(
            ((order_in, order_ref), (docs_in, docs_ref), (owner_in, owner_ref))
        )
    ]
    for copy in table_copies:
        copy.start()

    barrier = pltpu.get_barrier_semaphore()
    peers = quad + [far, pair, sibling]
    for peer in peers:
        pl.semaphore_signal(barrier, inc=1, device_id=peer, device_id_type=pl.DeviceIdType.MESH)
    pl.semaphore_wait(barrier, len(peers))

    targets = ((c, far), (across, quad[2]), (across_z, quad[1]), (across_y, quad[0]))

    for piece in range(pieces):
        pltpu.make_async_copy(stage.at[piece], stage.at[piece], stage_sem.at[piece]).wait()

    def first_send(piece, i):
        t, device = targets[i]
        remote(
            stage.at[piece, t],
            w_at(piece, q, x),
            init_send.at[piece],
            w_recv.at[piece, q],
            device,
        ).start()

    def arrive(piece, source):
        ref = w_at(piece, source, x)
        remote(ref, ref, init_send.at[0], w_recv.at[piece, source], sibling).wait_recv()

    def relay(piece, source, ssem, rsem, device):
        ref = w_at(piece, source, x)
        return remote(ref, ref, ssem, rsem, device)

    def some_rows(piece, count):
        return wbuf.at[piece, pl.ds(0, count * Rp)]

    def arrive_pair(piece, group, count):
        ref = some_rows(piece, count)
        remote(ref, ref, init_send.at[0], pair_recv.at[piece, group], sibling).wait_recv()

    near_sources = [g * A + t for t in (across_y, across_z, across)]
    far_sources = [(1 - g) * A + t for t in (c, across_y, across_z, across)]

    def pair_relay(piece, i):
        group = int(piece == pieces - 1 and i >= len(near_sources))
        relay(
            piece,
            (near_sources + far_sources)[i],
            pair_send.at[piece],
            pair_recv.at[piece, group],
            pair,
        ).start()

    def near_arrival(piece, i):
        source = near_sources[i]
        arrive(piece, source)
        relay(piece, source, far_send.at[piece], w_recv.at[piece, source], far).start()
        pair_relay(piece, i)

    def far_arrival(piece, i):
        arrive(piece, far_sources[i])
        pair_relay(piece, len(near_sources) + i)

    def token_rows(side, k):
        return pl.ds(pl.multiple_of(side * half + k * step, step), step)

    def token_copy(block, k, ssem, rsem, device):
        ref = normed.at[block, token_rows(d, k)]
        return remote(ref, ref, ssem, rsem, device)

    def own_copies(k):
        return (
            token_copy(c, k, own_send.at[0], tok_recv.at[0, k], quad[1]),
            token_copy(c, k, own_send.at[1], tok_recv.at[1, k], quad[0]),
            token_copy(c, k, own_send.at[2], sib_recv.at[0], sibling),
        )

    def pass_copy(k):
        return token_copy(across_z, k, pass_send.at[0], tok_recv.at[2, k], quad[0])

    token_blocks = (across_z, across_y, across)

    def share_copy(i, k):
        return token_copy(
            token_blocks[i], k, share_send.at[i], sib_recv.at[0], sibling
        )

    def token_arrival(i, k):
        ref = normed.at[token_blocks[i], token_rows(d, k)]
        remote(ref, ref, own_send.at[0], tok_recv.at[i, k], sibling).wait_recv()
        if i == 0:
            pass_copy(k).start()
        share_copy(i, k).start()

    def normalize(k):
        def block(i, carry):
            span = pl.ds(pl.multiple_of(k * step + i * 16, 16), 16)
            into = pl.ds(pl.multiple_of(d * half + k * step + i * 16, 16), 16)
            inputs = tokraw[span].astype(jnp.float32)
            mean = jnp.mean(inputs * inputs, -1, keepdims=True)
            normed[c, into] = (inputs * lax.rsqrt(mean + 1e-05) * gain[...]).astype(
                jnp.bfloat16
            )
            return carry

        lax.fori_loop(0, step // 16, block, 0)

    lane = lax.broadcasted_iota(jnp.int32, (rows, HD), 1)
    row_id = lax.broadcasted_iota(jnp.int32, (rows, 1), 0)

    def make_tables():
        step_angle = (row_id % blk).astype(jnp.float32) * freq[...]
        step_cos = jnp.cos(step_angle)
        step_sin = jnp.sin(step_angle)
        sign = jnp.where(lane < HD // 2, -1.0, 1.0)
        entry_id = lax.broadcasted_iota(jnp.int32, (A * slots, 1), 0)
        entries = jnp.zeros((A * slots, 1), jnp.int32)
        for k in range(A * slots):
            entries = jnp.where(entry_id == k, order_ref[g * A * slots + k], entries)
        base_angle = (entries * blk).astype(jnp.float32) * freq[...]
        base_cos = jnp.cos(base_angle)
        base_sin = jnp.sin(base_angle)
        for b in range(A):
            row_cos = jnp.broadcast_to(base_cos[b * slots : b * slots + 1], (rows, HD))
            row_sin = jnp.broadcast_to(base_sin[b * slots : b * slots + 1], (rows, HD))
            for i in range(1, slots):
                k = b * slots + i
                row_cos = jnp.where(row_id // blk == i, base_cos[k : k + 1], row_cos)
                row_sin = jnp.where(row_id // blk == i, base_sin[k : k + 1], row_sin)
            csbuf[0, b] = row_cos * step_cos - row_sin * step_sin
            csbuf[1, b] = (row_sin * step_cos + row_cos * step_sin) * sign

    def make_bias():
        key_id = lax.broadcasted_iota(jnp.int32, (1, T), 1)
        key_pos = jnp.zeros((1, T), jnp.int32)
        key_doc = jnp.zeros((1, T), jnp.int32)
        for i in range(T // blk):
            here = key_id // blk == i
            natural = order_ref[i]
            key_pos = jnp.where(here, natural * blk, key_pos)
            key_doc = jnp.where(here, docs_ref[natural], key_doc)
        key_pos = key_pos + key_id % blk

        def block(b, carry):
            first = jnp.zeros((rows, 1), jnp.int32)
            document = jnp.zeros((rows, 1), jnp.int32)
            for i in range(slots):
                natural = order_ref[(g * A + b) * slots + i]
                here = row_id // blk == i
                first = jnp.where(here, natural * blk, first)
                document = jnp.where(here, docs_ref[natural], document)
            allowed = (key_pos <= first + row_id % blk) & (key_doc == document)
            bias[b] = jnp.where(allowed, 0.0, -jnp.inf)
            return carry

        lax.fori_loop(0, A, block, 0)

    def pick_copies():
        mine = heads // 2
        count = picked.shape[1]
        into = pl.ds(pl.multiple_of(d * count, count), count)
        return (
            pltpu.make_async_copy(picked.at[0], cache_ref.at[into], cache_sem.at[0]),
            remote(
                picked.at[1], cache_ref.at[into], cache_sem.at[1], cache_sem.at[2], sibling
            ),
        )

    def pick_heads():
        prev_copy.wait()
        mine = heads // 2
        group = HD
        taken = group // 2
        out_id = lax.broadcasted_iota(jnp.int32, (taken, group), 0)
        in_id = lax.broadcasted_iota(jnp.int32, (taken, group), 1)
        for side in range(2):
            other = d if side == 0 else 1 - d
            wanted = jnp.zeros((taken, group), jnp.int32)
            for s in range(mine):
                wanted = jnp.where(out_id % mine == s, owner_ref[other * mine + s], wanted)
            chosen = (out_id // mine == in_id // heads) & (in_id % heads == wanted)
            selector = jnp.where(chosen, 1.0, 0.0).astype(jnp.bfloat16)
            for i in range(prev.shape[0] // group):
                picked[side, i * taken : (i + 1) * taken] = jnp.dot(
                    selector,
                    prev[i * group : (i + 1) * group],
                    preferred_element_type=jnp.float32,
                ).astype(jnp.bfloat16)
        for copy in pick_copies():
            copy.start()

    def turn(v, b):
        return v * csbuf[0, b] + pltpu.roll(v, HD // 2, 1) * csbuf[1, b]

    def kv_copy(n, side, b, device):
        ref = kvbuf.at[y, side * A + b]
        rsem = kv_recv.at[b] if n == 1 else kv_recv.at[A + n // 2]
        return remote(ref, ref, kv_send.at[n], rsem, device)

    def kv_arrivals(n):
        if n == 1:
            for b in range(A):
                ref = kvbuf.at[y, (1 - g) * A + b]
                remote(ref, ref, kv_send.at[0], kv_recv.at[b], sibling).wait_recv()
                kv_copy(2, 1 - g, b, quad[0]).start()
        else:
            side = g if n == 0 else 1 - g
            ref = kvbuf.at[1 - y, pl.ds(pl.multiple_of(side * A, A), A)]
            remote(
                ref, ref, kv_send.at[0], kv_recv.at[A + n // 2], sibling
            ).wait_recv()

    def project_kv(b, carry):
        raw = jnp.dot(normed[b], wbuf[0], preferred_element_type=jnp.float32)
        kvbuf[y, g * A + b] = jnp.where(y == 0, turn(raw, b), raw).astype(jnp.bfloat16)
        kv_copy(1, g, b, far).start()
        kv_copy(0, g, b, quad[0]).start()
        return carry

    def span_of(source, part):
        return pl.ds(pl.multiple_of(source * R + part * Rp, Rp), Rp)

    def partial(piece, b, spans):
        total = None
        for span in spans:
            term = jnp.dot(
                normed[b, :, span], wbuf[piece, span], preferred_element_type=jnp.float32
            )
            total = term if total is None else total + term
        return total

    scale = 1.0 / math.sqrt(HD)

    def att_copy(h, b):
        cols = pl.ds(pl.multiple_of((c * hpg + h) * HD, HD), HD)
        return remote(
            att.at[h, b],
            out_ref.at[:, cols],
            att_send.at[h],
            att_recv.at[0],
            dev(x, g * A + b, d),
        )

    def own_out(h):
        cols = pl.ds(pl.multiple_of((c * hpg + h) * HD, HD), HD)
        return pltpu.make_async_copy(att.at[h, c], out_ref.at[:, cols], out_sem.at[h])

    def order(s):
        back = A - 1 - s
        return near(back // 2, back % 2)

    def attend(h, pair_id, blocks, queries):
        scores = lax.dot_general(
            jnp.concatenate(queries, 0),
            kvbuf[0].reshape(T, HD),
            (((1,), (1,)), ((), ())),
            preferred_element_type=jnp.float32,
        ) * scale + jnp.concatenate([bias[b] for b in blocks], 0)
        weights = jnp.exp(scores - jnp.max(scores, -1, keepdims=True))
        total = jnp.sum(weights, -1, keepdims=True)
        weighted = jnp.dot(
            weights.astype(jnp.bfloat16),
            kvbuf[1].reshape(T, HD),
            preferred_element_type=jnp.float32,
        )
        done = (weighted / total).astype(jnp.bfloat16)
        for i, b in enumerate(blocks):
            att[h, b] = done[i * rows : (i + 1) * rows]
        att_copy(h, blocks[0]).start()

        @pl.when(pair_id < A // 2 - 1)
        def _():
            att_copy(h, blocks[1]).start()

    def attend_all(h, query):
        def attend_pair(s, carry):
            blocks = [order(2 * s), order(2 * s + 1)]
            attend(h, s, blocks, [query(b) for b in blocks])
            return carry

        lax.fori_loop(0, A // 2, attend_pair, 0)
        own_out(h).start()

    def own_tokens(k):
        if k == plan[0]:
            tok_copy.wait()
            gain_copy.wait()
        normalize(k)
        for copy in own_copies(k):
            copy.start()

    def spare(i):
        if i == first_spare:
            for copy in table_copies:
                copy.wait()
        if i:
            make_bias()
            pick_heads()
        else:
            freq_copy.wait()
            make_tables()

    def start_keys():
        ref = normed.at[pl.ds(0, A // 2)]
        remote(ref, ref, own_send.at[0], sib_recv.at[0], sibling).wait_recv()
        for piece in range(pieces):
            pltpu.make_async_copy(
                own_rows(piece), own_rows(piece), local_sem.at[piece]
            ).wait()
        arrive_pair(0, 0, len(near_sources) + len(far_sources))
        lax.fori_loop(0, A, project_kv, 0)

    def project_first():
        arrive_pair(1, 0, len(near_sources) + len(far_sources))

        def project(s, carry):
            b = order(s)
            product = jnp.dot(normed[b], wbuf[1], preferred_element_type=jnp.float32)
            qbuf[b] = turn(product, b).astype(jnp.bfloat16)
            return carry

        lax.fori_loop(0, A, project, 0)

    def attend_first():
        attend_all(0, lambda b: qbuf[b])

    last = hpg
    near_count, far_count = len(near_sources), len(far_sources)

    def project_early():
        early = [span_of(q, 0), span_of(q, 1)]
        early += [span_of(source, x) for source in near_sources]

        def project(b, carry):
            acc[b] = partial(last, b, early)
            return carry

        lax.fori_loop(0, A, project, 0)

    def attend_last():
        arrive_pair(last, 0, near_count)
        middle = [span_of(source, 1 - x) for source in near_sources]
        middle += [span_of(source, x) for source in far_sources]

        def project(b, carry):
            acc[b] += partial(last, b, middle)
            return carry

        lax.fori_loop(0, A, project, 0)
        arrive_pair(last, 1, far_count)
        late = [span_of(source, 1 - x) for source in far_sources]

        def query(b):
            return turn(acc[b] + partial(last, b, late), b).astype(jnp.bfloat16)

        attend_all(1, query)

    steps = {
        "first": first_send,
        "near": near_arrival,
        "far": far_arrival,
        "own": own_tokens,
        "tok": token_arrival,
        "spare": spare,
        "keys": start_keys,
        "kv": kv_arrivals,
        "query": project_first,
        "head": attend_first,
        "early": project_early,
        "last": attend_last,
    }
    first_spare = [where[0] for name, *where in plan[1] if name == "spare"][0]
    for name, *where in plan[1]:
        steps[name](*where)

    def drain(ref, sem):
        remote(ref, ref, sem, w_recv.at[0, q], far).wait_send()

    for piece in range(pieces):
        drain(some_rows(piece, A), init_send.at[piece])
        drain(some_rows(piece, near_count), far_send.at[piece])
        drain(some_rows(piece, near_count + far_count), pair_send.at[piece])
    half_rows = normed.at[0, pl.ds(0, half)]
    for sem in (*(own_send.at[i] for i in range(3)), pass_send.at[0]):
        drain(half_rows, sem)
    for i in range(len(token_blocks)):
        drain(half_rows, share_send.at[i])
    for n in range(3):
        drain(kvbuf.at[0, pl.ds(0, A)], kv_send.at[n])
    local_pick, sent_pick = pick_copies()
    local_pick.wait()
    sent_pick.wait()
    for h in range(hpg):
        own_out(h).wait()
        drain(att.at[h, pl.ds(0, A - 1)], att_send.at[h])
    ref = kvbuf.at[0, pl.ds(0, hpg * (A - 1))]
    remote(ref, ref, own_send.at[0], att_recv.at[0], sibling).wait_recv()


def quad_plan(
    tokens, norm_gain, w_query, w_key, w_value, block_order, block_docs, head_owner, prev_kv
):
    n_seq = lax.axis_size("seq")
    rows, width = tokens.shape
    R = w_query.shape[0]
    local_kv = w_key.shape[1] // HD
    local_heads = w_query.shape[1] // HD
    A = 2 * local_kv
    hpg = local_heads // A
    slots = block_order.shape[0] // n_seq
    blk = rows // slots
    T = n_seq * rows
    owned = [where[0] for name, *where in PLAN if name == "own"]
    first_own, chunks = owned[0], len(owned)
    kept, planes, heads, _ = prev_kv.shape
    count = kept * planes * (heads // 2)
    frequency = 500000.0 ** (-np.arange(HD // 2, dtype=np.float64) / (HD // 2))
    freq = np.concatenate([frequency, frequency]).astype(np.float32)[None, :]
    sizes = (A, rows, R, hpg, slots, blk, T, chunks, heads)
    pieces = hpg + 1
    dma = pltpu.SemaphoreType.DMA
    anywhere = pl.BlockSpec(memory_space=pl.ANY)
    bf16, f32 = jnp.bfloat16, jnp.float32
    attended, cache = pl.pallas_call(
        functools.partial(quad_kernel, (first_own, PLAN), sizes),
        out_shape=(
            pltpu.VMEM((rows, local_heads * HD), bf16),
            pltpu.VMEM((2 * count, HD), prev_kv.dtype),
        ),
        in_specs=[anywhere] * 10,
        out_specs=(anywhere, anywhere),
        scratch_shapes=[
            pltpu.SMEM(block_order.shape, jnp.int32),
            pltpu.SMEM(block_docs.shape, jnp.int32),
            pltpu.SMEM(head_owner.shape, jnp.int32),
            pltpu.VMEM((pieces, A, R // 2, HD), bf16),
            pltpu.VMEM((1, HD), f32),
            pltpu.VMEM((1, width), f32),
            pltpu.VMEM((rows // 2, width), bf16),
            pltpu.VMEM((pieces, width, HD), bf16),
            pltpu.VMEM((A, rows, width), bf16),
            pltpu.VMEM((A, rows, HD), bf16),
            pltpu.VMEM((A, rows, HD), f32),
            pltpu.VMEM((2, n_seq, rows, HD), bf16),
            pltpu.VMEM((2, A, rows, HD), f32),
            pltpu.VMEM((A, rows, T), f32),
            pltpu.VMEM((hpg, A, rows, HD), bf16),
            pltpu.VMEM((kept * planes * heads, HD), bf16),
            pltpu.VMEM((2, count, HD), bf16),
            dma((pieces + 4,)),
            dma((pieces,)),
            dma((3,)),
            dma((pieces,)),
            dma((pieces,)),
            dma((pieces,)),
            dma((pieces, n_seq)),
            dma((pieces, 2)),
            dma((3,)),
            dma((1,)),
            dma((3,)),
            dma((3, chunks)),
            dma((1,)),
            dma((3,)),
            dma((A + 2,)),
            dma((hpg,)),
            dma((1,)),
            dma((hpg,)),
            dma((3,)),
        ],
        compiler_params=pltpu.CompilerParams(collective_id=1, has_side_effects=True),
    )(
        block_order,
        block_docs,
        head_owner,
        freq,
        norm_gain[None, :],
        tokens,
        w_query,
        w_key,
        w_value,
        prev_kv.reshape(kept * planes * heads, HD),
    )
    return attended, cache.reshape(2 * kept, planes, heads // 2, HD)


def solution(mesh):
    in_specs = (
        P(("groups", "seq"), None),
        P(),
        P("seq", "dec"),
        P("seq", "dec"),
        P("seq", "dec"),
        P("groups"),
        P("groups"),
        P("groups"),
        P(("groups", "seq", "dec"), None, None, None),
    )
    out_specs = (P(("groups", "seq"), "dec"), P(("groups", "seq"), None, "dec", None))
    X = mesh.shape["groups"]
    n_seq = mesh.shape["seq"]

    def per_device(tokens, norm_gain, w_query, w_key, w_value, *rest):
        A = 2 * (w_key.shape[1] // HD)
        heads = w_query.shape[1] // HD
        fits = (
            mesh.shape["dec"] == 2
            and A & (A - 1) == 0
            and n_seq % A == 0
            and heads % A == 0
            and w_query.shape[0] % (16 * X) == 0
            and tokens.shape[0] % 32 == 0
        )
        squared = (
            fits
            and A == 4
            and X == 2
            and n_seq == 2 * A
            and heads == 2 * A
            and tokens.shape[0] % 128 == 0
            and rest[-1].shape[3] == HD
            and HD % (2 * rest[-1].shape[2]) == 0
            and (rest[-1].shape[0] * rest[-1].shape[1] * rest[-1].shape[2]) % HD == 0
        )
        plan = functools.partial(column_plan, X) if fits else general_plan
        plan = quad_plan if squared else plan
        return plan(tokens, norm_gain, w_query, w_key, w_value, *rest)

    return jax.shard_map(
        per_device, mesh=mesh, in_specs=in_specs, out_specs=out_specs, check_vma=False
    )
```

```python
import functools
import math

import jax
import jax.numpy as jnp
import numpy as np
from jax import lax
from jax.experimental import pallas as pl
from jax.experimental.pallas import tpu as pltpu
from jax.sharding import PartitionSpec as P

HD = 128


def rotate(values, positions):
    half_width = values.shape[-1] // 2
    frequency = 500000.0 ** (-jnp.arange(half_width, dtype=jnp.float32) / half_width)
    angles = positions[:, None].astype(jnp.float32) * frequency[None, :]
    cosines = jnp.cos(angles)[:, None, :]
    sine_terms = jnp.sin(angles)[:, None, :]
    lower_half = values[..., :half_width]
    upper_half = values[..., half_width:]
    return jnp.concatenate(
        [
            lower_half * cosines - upper_half * sine_terms,
            upper_half * cosines + lower_half * sine_terms,
        ],
        -1,
    )


def general_plan(
    tokens, norm_gain, w_query, w_key, w_value, block_order, block_docs, head_owner, prev_kv
):
    rows_dev = tokens.shape[0]
    block_rows = rows_dev // 2
    inputs = tokens.astype(jnp.float32)
    normed = (
        inputs * lax.rsqrt(jnp.mean(inputs * inputs, -1, keepdims=True) + 1e-05) * norm_gain
    ).astype(jnp.bfloat16)

    def add_piece(piece):
        return jnp.dot(normed, piece, preferred_element_type=jnp.float32)

    pieces = (
        lax.all_gather(w_query, "seq", axis=0, tiled=True),
        lax.all_gather(w_key, "seq", axis=0, tiled=True),
        lax.all_gather(w_value, "seq", axis=0, tiled=True),
    )
    query_full, key_full, value_full = tuple((add_piece(piece) for piece in pieces))
    total_rows = rows_dev * lax.axis_size("seq")
    row_ids = jnp.arange(total_rows, dtype=jnp.int32)
    natural = jnp.take(block_order, row_ids // block_rows)
    pos_all = natural * block_rows + row_ids % block_rows
    doc_all = jnp.take(block_docs, natural)
    offset = lax.axis_index("seq") * rows_dev
    my_pos = lax.dynamic_slice_in_dim(pos_all, offset, rows_dev)
    my_doc = lax.dynamic_slice_in_dim(doc_all, offset, rows_dev)
    local_kv = key_full.shape[1] // HD
    local_heads = query_full.shape[1] // HD
    group_size = local_heads // local_kv
    queries = rotate(query_full.reshape(rows_dev, local_heads, HD), my_pos).astype(jnp.bfloat16)
    query_groups = queries.reshape(rows_dev, local_kv, group_size, HD).transpose(1, 2, 0, 3)
    key_rows = (
        rotate(key_full.reshape(rows_dev, local_kv, HD), my_pos)
        .astype(jnp.bfloat16)
        .reshape(rows_dev, local_kv * HD)
    )
    value_rows = value_full.astype(jnp.bfloat16)
    scale = 1.0 / math.sqrt(HD)
    start_max = jnp.full((local_kv, group_size, rows_dev, 1), -jnp.inf, jnp.float32)
    start_sum = jnp.zeros((local_kv, group_size, rows_dev, 1), jnp.float32)
    start_weighted = jnp.zeros((local_kv, group_size, rows_dev, HD), jnp.float32)
    key_piece = lax.all_gather(key_rows, "seq", axis=0, tiled=True)
    value_piece = lax.all_gather(value_rows, "seq", axis=0, tiled=True)
    count = key_piece.shape[0]
    allowed = (pos_all[None, :] <= my_pos[:, None]) & (doc_all[None, :] == my_doc[:, None])

    def update(state):
        running_max, running_sum, weighted = state
        scores = (
            jnp.einsum(
                "ghtd,sgd->ghts",
                query_groups,
                key_piece.reshape(count, local_kv, HD),
                preferred_element_type=jnp.float32,
            )
            * scale
        )
        scores = jnp.where(allowed, scores, -jnp.inf)
        new_max = jnp.max(scores, -1, keepdims=True)
        shift_by = jnp.where(new_max == -jnp.inf, 0.0, new_max)
        weights = jnp.exp(scores - shift_by)
        rescale = jnp.exp(running_max - shift_by)
        running_sum = running_sum * rescale + jnp.sum(weights, -1, keepdims=True)
        weighted = weighted * rescale + jnp.einsum(
            "ghts,sgd->ghtd",
            weights.astype(jnp.bfloat16),
            value_piece.reshape(count, local_kv, HD),
            preferred_element_type=jnp.float32,
        )
        return (new_max, running_sum, weighted)

    final_max, final_sum, final_weighted = lax.cond(
        jnp.any(allowed), update, lambda state: state, (start_max, start_sum, start_weighted)
    )
    attended = (
        (final_weighted / final_sum)
        .transpose(2, 0, 1, 3)
        .reshape(rows_dev, local_heads * HD)
        .astype(jnp.bfloat16)
    )
    head_count = prev_kv.shape[2]
    selector = (head_owner[:, None] == jnp.arange(head_count, dtype=jnp.int32)[None, :]).astype(
        jnp.bfloat16
    )
    ordered = jnp.einsum(
        "tcjd,sj->tcsd", prev_kv, selector, preferred_element_type=jnp.float32
    ).astype(jnp.bfloat16)
    decode_cache = lax.all_to_all(ordered, "dec", split_axis=2, concat_axis=0, tiled=True)
    return (attended, decode_cache)


def attend_kernel(
    sizes,
    order_ref,
    docs_ref,
    freq_ref,
    gain_ref,
    tok_in,
    wq_in,
    wk_in,
    wv_in,
    prev_in,
    out_ref,
    prev_out,
    tok,
    wbuf,
    normed,
    qbuf,
    kvbuf,
    csbuf,
    att,
    local_sem,
    home_send,
    homeq_recv,
    homekv_recv,
    rel_send,
    rel_recv,
    own_send,
    fwd_send,
    tok_recv,
    sib_send,
    sib_recv,
    prev_sem,
    kv_send,
    kv_recv,
    att_send,
    att_recv,
):
    X, A, Y, rows, R, hpg, slots, blk, T = sizes
    Rp = R // X
    half = rows // 2
    QW = hpg * HD
    x = lax.axis_index("groups")
    q = lax.axis_index("seq")
    d = lax.axis_index("dec")
    a = q // Y
    y = q % Y
    unit = a % 2

    def dev(x_, a_, y_, d_=None):
        return {"groups": x_, "seq": a_ * Y + y_, "dec": d if d_ is None else d_}

    def remote(src, dst, ssem, rsem, device):
        return pltpu.make_async_remote_copy(
            src_ref=src,
            dst_ref=dst,
            send_sem=ssem,
            recv_sem=rsem,
            device_id=device,
            device_id_type=pl.DeviceIdType.MESH,
        )

    sibling = dev(x, a, y, 1 - d)
    barrier = pltpu.get_barrier_semaphore()
    plane = [(i, j) for i in range(X) for j in range(Y) if (i, j) != (0, 0)]
    peers = [dev((x + i) % X, a, (y + j) % Y) for i, j in plane]
    peers += [dev(x, (a + t) % A, y) for t in range(1, A)]
    mate = a + 1 - 2 * unit
    peers += [dev(x, mate, (y + j) % Y) for j in range(1, Y)]
    peers.append(sibling)
    for peer in peers:
        pl.semaphore_signal(barrier, inc=1, device_id=peer, device_id_type=pl.DeviceIdType.MESH)
    pl.semaphore_wait(barrier, len(peers))

    def w_rows(a_, y_, x_):
        return pl.ds(pl.multiple_of((a_ * Y + y_) * R + x_ * Rp, Rp), Rp)

    part = pl.ds(pl.multiple_of(x * Rp, Rp), Rp)

    def kv_source(t):
        return wv_in if t % 2 else wk_in

    def home_copies(t):
        kv_cols = pl.ds((t // 2) * HD, HD)
        return (
            remote(
                wq_in.at[part, pl.ds(t * QW, QW)],
                wbuf.at[w_rows(a, y, x), pl.ds(0, QW)],
                home_send.at[0, t],
                homeq_recv.at[a],
                dev(x, t, y),
            ),
            remote(
                kv_source(t).at[part, kv_cols],
                wbuf.at[w_rows(a, y, x), pl.ds(QW, HD)],
                home_send.at[1, t],
                homekv_recv.at[a],
                dev(x, t, y),
            ),
        )

    def local_copies(t):
        rows_all = pl.ds(pl.multiple_of(q * R, R), R)
        return (
            pltpu.make_async_copy(
                wq_in.at[:, pl.ds(t * QW, QW)],
                wbuf.at[rows_all, pl.ds(0, QW)],
                local_sem.at[0],
            ),
            pltpu.make_async_copy(
                kv_source(t).at[:, pl.ds((t // 2) * HD, HD)],
                wbuf.at[rows_all, pl.ds(QW, HD)],
                local_sem.at[1],
            ),
        )

    for t in range(A):

        @pl.when(a == t)
        def _():
            for copy in local_copies(t):
                copy.start()

        @pl.when(a != t)
        def _():
            for copy in home_copies(t):
                copy.start()

    my_half = pl.ds(pl.multiple_of(d * half, half), half)
    other_half = pl.ds(pl.multiple_of((1 - d) * half, half), half)

    def own_push(side):
        return remote(
            tok_in.at[my_half],
            tok.at[a, my_half],
            own_send.at[side],
            tok_recv.at[a],
            dev(x, a + 1 - 2 * side, y),
        )

    @pl.when(a + 1 < A)
    def _():
        own_push(0).start()

    @pl.when(a >= 1)
    def _():
        own_push(1).start()

    own_tok = pltpu.make_async_copy(tok_in, tok.at[a], local_sem.at[2])
    own_tok.start()
    prev_copy = remote(prev_in, prev_out, prev_sem.at[0], prev_sem.at[1], sibling)
    prev_copy.start()

    def relay(t, index, i, j):
        src = wbuf.at[w_rows(t, y, x)]
        return remote(
            src,
            src,
            rel_send.at[t, index],
            rel_recv.at[t, y, x],
            dev((x + i) % X, a, (y + j) % Y),
        )

    for t in range(A):

        @pl.when(a == t)
        def _():
            for copy in local_copies(t):
                copy.wait()
            for index, (i, j) in enumerate(plane):
                if j:
                    relay(t, index, i, j).start()

    lane = lax.broadcasted_iota(jnp.int32, (rows, HD), 1)
    row_id = lax.broadcasted_iota(jnp.int32, (rows, 1), 0)

    def row_values(c, table):
        value = jnp.zeros((rows, 1), jnp.int32)
        for i in range(slots):
            entry = table(order_ref[(c * Y + y) * slots + i])
            value = jnp.where(row_id // blk == i, entry, value)
        return value

    def row_positions(c):
        return row_values(c, lambda n: n) * blk + row_id % blk

    for o in range(1, A):
        t = (a + o) % A
        src = wbuf.at[w_rows(t, y, x)]
        remote(
            wq_in.at[part, pl.ds(0, QW)],
            wbuf.at[w_rows(t, y, x), pl.ds(0, QW)],
            home_send.at[0, 0],
            homeq_recv.at[t],
            sibling,
        ).wait_recv()
        remote(
            wk_in.at[part, pl.ds(0, HD)],
            wbuf.at[w_rows(t, y, x), pl.ds(QW, HD)],
            home_send.at[1, 0],
            homekv_recv.at[t],
            sibling,
        ).wait_recv()
        for index, (i, j) in enumerate(plane):
            relay(t, index, i, j).start()

    def forward(c, to):
        return remote(
            tok.at[c, my_half],
            tok.at[c, my_half],
            fwd_send.at[c],
            tok_recv.at[c],
            dev(x, to, y),
        )

    def share(c):
        return remote(
            tok.at[c, my_half], tok.at[c, my_half], sib_send.at[c], sib_recv.at[c], sibling
        )

    def token_step(s):
        @pl.when(a >= s)
        def _():
            c = a - s
            forward(c, a).wait_recv()

            @pl.when(a + 1 < A)
            def _():
                forward(c, a + 1).start()

            share(c).start()

        @pl.when(a + s < A)
        def _():
            c = a + s
            forward(c, a).wait_recv()

            @pl.when(a >= 1)
            def _():
                forward(c, a - 1).start()

            share(c).start()

    def pick(s):
        value, bit = 0, 1
        while bit < A:
            value = value + bit * ((a // bit + s // bit) % 2)
            bit *= 2
        return value

    def kv_peer(dy, da):
        return dev(x, a - unit + (unit + da) % 2, (y + dy) % Y)

    kv_plan = [(dy, da) for dy in range(Y) for da in range(2) if (dy, da) != (0, 0)]

    def kv_push(s, c, index, dy, da):
        src = kvbuf.at[unit, c * Y + y]
        return remote(src, src, kv_send.at[s, index], kv_recv.at[unit, c, y], kv_peer(dy, da))

    def normalize(s):
        c = pick(s)
        if s == 0:
            own_tok.wait()
        else:
            other = tok.at[c, other_half]
            remote(other, other, sib_send.at[c], sib_recv.at[c], sibling).wait_recv()

        def block(i, carry):
            span = pl.ds(pl.multiple_of(i * 16, 16), 16)
            inputs = tok[c, span].astype(jnp.float32)
            mean = jnp.mean(inputs * inputs, -1, keepdims=True)
            normed[c, span] = (inputs * lax.rsqrt(mean + 1e-05) * gain_ref[...]).astype(
                jnp.bfloat16
            )
            return carry

        lax.fori_loop(0, rows // 16, block, 0, unroll=2)

    def project(s, carry):
        c = pick(s)
        cosine = csbuf[0, c]
        sine = csbuf[1, c]

        def turn(v):
            return v * cosine + pltpu.roll(v, HD // 2, 1) * sine

        raw = jnp.dot(normed[c], wbuf[:, QW:], preferred_element_type=jnp.float32)
        kvbuf[unit, c * Y + y] = jnp.where(unit == 0, turn(raw), raw).astype(jnp.bfloat16)
        product = jnp.dot(normed[c], wbuf[:, :QW], preferred_element_type=jnp.float32)
        for index, (dy, da) in enumerate(kv_plan):
            kv_push(s, c, index, dy, da).start()
        for h in range(hpg):
            qbuf[c, :, h * HD : (h + 1) * HD] = turn(product[:, h * HD : (h + 1) * HD]).astype(
                jnp.bfloat16
            )
        return carry

    step_angle = (row_id % blk).astype(jnp.float32) * freq_ref[...]
    step_cos = jnp.cos(step_angle)
    step_sin = jnp.sin(step_angle)
    sign = jnp.where(lane < HD // 2, -1.0, 1.0)
    entry_id = lax.broadcasted_iota(jnp.int32, (A * slots, 1), 0)
    entries = jnp.zeros((A * slots, 1), jnp.int32)
    for c in range(A):
        for i in range(slots):
            entries = jnp.where(
                entry_id == c * slots + i, order_ref[(c * Y + y) * slots + i], entries
            )
    base_angle = (entries * blk).astype(jnp.float32) * freq_ref[...]
    base_cos = jnp.cos(base_angle)
    base_sin = jnp.sin(base_angle)
    for c in range(A):
        row_cos = jnp.broadcast_to(base_cos[c * slots : c * slots + 1], (rows, HD))
        row_sin = jnp.broadcast_to(base_sin[c * slots : c * slots + 1], (rows, HD))
        for i in range(1, slots):
            k = c * slots + i
            row_cos = jnp.where(row_id // blk == i, base_cos[k : k + 1], row_cos)
            row_sin = jnp.where(row_id // blk == i, base_sin[k : k + 1], row_sin)
        csbuf[0, c] = row_cos * step_cos - row_sin * step_sin
        csbuf[1, c] = (row_sin * step_cos + row_cos * step_sin) * sign

    normalize(0)
    for s in range(1, A - 1):
        token_step(s)
        normalize(s)
    for o in range(A):
        t = (a + o) % A
        for i, j in plane:
            if o or j:
                src = wbuf.at[w_rows(t, (y + j) % Y, (x + i) % X)]
                remote(
                    src,
                    src,
                    rel_send.at[0, 0],
                    rel_recv.at[t, (y + j) % Y, (x + i) % X],
                    sibling,
                ).wait_recv()

    lax.fori_loop(0, A - 1, project, 0)
    token_step(A - 1)
    normalize(A - 1)
    project(A - 1, 0)

    for s in range(A):
        c = pick(s)
        for dy, da in kv_plan:
            u = (unit + da) % 2
            dst = kvbuf.at[u, c * Y + (y + dy) % Y]
            remote(
                dst, dst, kv_send.at[0, 0], kv_recv.at[u, c, (y + dy) % Y], sibling
            ).wait_recv()

    key_id = lax.broadcasted_iota(jnp.int32, (1, T), 1)
    key_pos = jnp.zeros((1, T), jnp.int32)
    key_doc = jnp.zeros((1, T), jnp.int32)
    for i in range(T // blk):
        here = key_id // blk == i
        natural = order_ref[i]
        key_pos = jnp.where(here, natural * blk, key_pos)
        key_doc = jnp.where(here, docs_ref[natural], key_doc)
    key_pos = key_pos + key_id % blk
    scale = 1.0 / math.sqrt(HD)
    out_cols = pl.ds(pl.multiple_of(a * QW, QW), QW)

    def att_push(s, c):
        return remote(
            att.at[c], out_ref.at[:, out_cols], att_send.at[s], att_recv.at[a], dev(x, c, y)
        )

    def attend(s, carry):
        c = pick(A - 1 - s)
        allowed = (key_pos <= row_positions(c)) & (
            key_doc == row_values(c, lambda n: docs_ref[n])
        )
        keys = kvbuf[0].reshape(T, HD)
        values = kvbuf[1].reshape(T, HD)
        for h in range(hpg):
            scores = (
                lax.dot_general(
                    qbuf[c, :, h * HD : (h + 1) * HD],
                    keys,
                    (((1,), (1,)), ((), ())),
                    preferred_element_type=jnp.float32,
                )
                * scale
            )
            scores = jnp.where(allowed, scores, -jnp.inf)
            weights = jnp.exp(scores - jnp.max(scores, -1, keepdims=True))
            total = jnp.sum(weights, -1, keepdims=True)
            weighted = jnp.dot(
                weights.astype(jnp.bfloat16), values, preferred_element_type=jnp.float32
            )
            att[c, :, h * HD : (h + 1) * HD] = (weighted / total).astype(jnp.bfloat16)

        @pl.when(s < A - 1)
        def _():
            att_push(s, c).start()

        return carry

    lax.fori_loop(0, A, attend, 0)
    own_out = pltpu.make_async_copy(att.at[a], out_ref.at[:, out_cols], local_sem.at[3])
    own_out.start()

    for t in range(A):

        @pl.when(a != t)
        def _():
            for copy in home_copies(t):
                copy.wait_send()
            for index, (i, j) in enumerate(plane):
                relay(t, index, i, j).wait_send()

        @pl.when(a == t)
        def _():
            for index, (i, j) in enumerate(plane):
                if j:
                    relay(t, index, i, j).wait_send()

    @pl.when(a + 1 < A)
    def _():
        own_push(0).wait_send()

    @pl.when(a >= 1)
    def _():
        own_push(1).wait_send()

    for s in range(1, A):

        @pl.when(a >= s)
        def _():
            share(a - s).wait_send()

            @pl.when(a + 1 < A)
            def _():
                forward(a - s, a + 1).wait_send()

        @pl.when(a + s < A)
        def _():
            share(a + s).wait_send()

            @pl.when(a >= 1)
            def _():
                forward(a + s, a - 1).wait_send()

    for s in range(A):
        for index, (dy, da) in enumerate(kv_plan):
            kv_push(s, pick(s), index, dy, da).wait_send()
    prev_copy.wait()
    own_out.wait()
    for s in range(A - 1):
        att_push(s, pick(A - 1 - s)).wait_send()
    for o in range(1, A):
        t = (a + o) % A
        cols = pl.ds(pl.multiple_of(t * QW, QW), QW)
        remote(
            att.at[0], out_ref.at[:, cols], att_send.at[0], att_recv.at[t], sibling
        ).wait_recv()


def column_plan(
    X, tokens, norm_gain, w_query, w_key, w_value, block_order, block_docs, head_owner, prev_kv
):
    n_seq = lax.axis_size("seq")
    rows, width = tokens.shape
    R = w_query.shape[0]
    local_kv = w_key.shape[1] // HD
    local_heads = w_query.shape[1] // HD
    A = 2 * local_kv
    Y = n_seq // A
    hpg = local_heads // A
    slots = block_order.shape[0] // n_seq
    blk = rows // slots
    T = n_seq * rows
    QW = hpg * HD
    frequency = 500000.0 ** (-jnp.arange(HD // 2, dtype=jnp.float32) / (HD // 2))
    freq = jnp.concatenate([frequency, frequency])[None, :]
    sizes = (X, A, Y, rows, R, hpg, slots, blk, T)
    dma = pltpu.SemaphoreType.DMA
    smem = pl.BlockSpec(memory_space=pltpu.SMEM)
    vmem = pl.BlockSpec(memory_space=pltpu.VMEM)
    anywhere = pl.BlockSpec(memory_space=pl.ANY)
    attended, other = pl.pallas_call(
        functools.partial(attend_kernel, sizes),
        out_shape=(
            jax.ShapeDtypeStruct((rows, local_heads * HD), jnp.bfloat16),
            jax.ShapeDtypeStruct(prev_kv.shape, prev_kv.dtype),
        ),
        in_specs=[smem, smem, vmem, vmem] + [anywhere] * 5,
        out_specs=(vmem, anywhere),
        scratch_shapes=[
            pltpu.VMEM((A, rows, width), jnp.bfloat16),
            pltpu.VMEM((width, QW + HD), jnp.bfloat16),
            pltpu.VMEM((A, rows, width), jnp.bfloat16),
            pltpu.VMEM((A, rows, QW), jnp.bfloat16),
            pltpu.VMEM((2, n_seq, rows, HD), jnp.bfloat16),
            pltpu.VMEM((2, A, rows, HD), jnp.float32),
            pltpu.VMEM((A, rows, QW), jnp.bfloat16),
            dma((4,)),
            dma((2, A)),
            dma((A,)),
            dma((A,)),
            dma((A, X * Y)),
            dma((A, Y, X)),
            dma((2,)),
            dma((A,)),
            dma((A,)),
            dma((A,)),
            dma((A,)),
            dma((2,)),
            dma((A, 2 * Y)),
            dma((2, A, Y)),
            dma((A,)),
            dma((A,)),
        ],
        compiler_params=pltpu.CompilerParams(
            collective_id=0, has_side_effects=True
        ),
    )(
        block_order,
        block_docs,
        freq,
        norm_gain[None, :],
        tokens,
        w_query,
        w_key,
        w_value,
        prev_kv,
    )
    d = lax.axis_index("dec")
    head_count = prev_kv.shape[2]
    mine = head_count // 2
    owner = lax.dynamic_slice_in_dim(head_owner, d * mine, mine)
    both = jnp.concatenate(
        [jnp.where(d == 0, prev_kv, other), jnp.where(d == 0, other, prev_kv)], 0
    )
    picks = []
    for s in range(mine):
        chosen = both[:, :, 0]
        for j in range(1, head_count):
            chosen = jnp.where(owner[s] == j, both[:, :, j], chosen)
        picks.append(chosen)
    return attended, jnp.stack(picks, 2)


PLAN = (
    ("first", 2, 3), ("first", 1, 3), ("first", 0, 1), ("first", 0, 2), ("first", 0, 0),
    ("own", 1), ("first", 0, 3), ("near", 0, 1), ("far", 0, 0), ("own", 2), ("near", 1, 0),
    ("own", 0), ("tok", 0, 2), ("near", 0, 2), ("near", 0, 0), ("first", 1, 2),
    ("first", 1, 1), ("first", 1, 0), ("tok", 1, 2), ("own", 3), ("first", 2, 1),
    ("tok", 0, 0), ("far", 0, 3), ("tok", 0, 1), ("near", 2, 0), ("spare", 1), ("near", 1, 1),
    ("first", 2, 0), ("far", 0, 2), ("far", 0, 1), ("far", 1, 0), ("near", 1, 2),
    ("tok", 0, 3), ("first", 2, 2), ("far", 2, 1), ("tok", 2, 3), ("near", 2, 2),
    ("tok", 2, 1), ("tok", 2, 0), ("spare", 0), ("tok", 1, 3), ("tok", 2, 2), ("tok", 1, 1),
    ("tok", 1, 0), ("far", 1, 2), ("far", 1, 1), ("keys",), ("near", 2, 1), ("early", 1, 0),
    ("far", 1, 3), ("far", 2, 0), ("early", 2, 0), ("early", 1, 1), ("far", 2, 3), ("kv", 1),
    ("query",), ("far", 2, 2), ("early", 2, 1), ("kv", 0), ("kv", 2), ("head",), ("last",),
)


def quad_kernel(
    plan,
    sizes,
    order_in,
    docs_in,
    owner_in,
    freq_in,
    gain_in,
    tok_in,
    wq_in,
    wk_in,
    wv_in,
    prev_in,
    out_ref,
    cache_ref,
    order_ref,
    docs_ref,
    owner_ref,
    stage,
    freq,
    gain,
    tokraw,
    wbuf,
    normed,
    qbuf,
    acc,
    kvbuf,
    csbuf,
    bias,
    att,
    prev,
    picked,
    local_sem,
    stage_sem,
    table_sem,
    init_send,
    far_send,
    pair_send,
    w_recv,
    pair_recv,
    own_send,
    pass_send,
    share_send,
    tok_recv,
    sib_recv,
    kv_send,
    kv_recv,
    att_send,
    att_recv,
    out_sem,
    cache_sem,
):
    A, rows, R, hpg, slots, blk, T, chunks, heads = sizes
    Rp = R // 2
    half = rows // 2
    step = half // chunks
    x = lax.axis_index("groups")
    q = lax.axis_index("seq")
    d = lax.axis_index("dec")
    g = q // A
    c = q % A
    u = c // 2
    y = c % 2

    def near(du, dy):
        return ((u + du) % 2) * 2 + (y + dy) % 2

    across_y, across_z, across = near(0, 1), near(1, 0), near(1, 1)

    def dev(x_, q_, d_):
        return {"groups": x_, "seq": q_, "dec": d_}

    def remote(src, dst, ssem, rsem, device):
        return pltpu.make_async_remote_copy(
            src_ref=src,
            dst_ref=dst,
            send_sem=ssem,
            recv_sem=rsem,
            device_id=device,
            device_id_type=pl.DeviceIdType.MESH,
        )

    sibling = dev(x, q, 1 - d)
    pair = dev(1 - x, q, d)
    far = dev(x, (1 - g) * A + c, d)
    quad = [dev(x, g * A + t, d) for t in (across_y, across_z, across)]

    barrier = pltpu.get_barrier_semaphore()
    peers = quad + [far, pair, sibling]
    for peer in peers:
        pl.semaphore_signal(barrier, inc=1, device_id=peer, device_id_type=pl.DeviceIdType.MESH)

    def w_at(piece, source, part):
        return wbuf.at[piece, pl.ds(pl.multiple_of(source * R + part * Rp, Rp), Rp)]

    part_rows = pl.ds(pl.multiple_of(x * Rp, Rp), Rp)

    def weights(piece, t):
        if piece:
            return wq_in, (t * hpg + piece - 1) * HD
        return (wv_in if t % 2 else wk_in), (t // 2) * HD

    pieces = hpg + 1
    my_half = pl.ds(pl.multiple_of(d * half, half), half)
    tok_copy = pltpu.make_async_copy(tok_in.at[my_half], tokraw, local_sem.at[pieces])
    tok_copy.start()
    gain_copy = pltpu.make_async_copy(gain_in, gain, local_sem.at[pieces + 1])
    gain_copy.start()
    freq_copy = pltpu.make_async_copy(freq_in, freq, local_sem.at[pieces + 2])
    freq_copy.start()
    prev_copy = pltpu.make_async_copy(prev_in, prev, local_sem.at[pieces + 3])
    prev_copy.start()

    def own_rows(piece):
        return wbuf.at[piece, pl.ds(pl.multiple_of(q * R, R), R)]

    def own_copy(piece, t):
        source, column = weights(piece, t)
        return pltpu.make_async_copy(
            source.at[:, pl.ds(column, HD)], own_rows(piece), local_sem.at[piece]
        )

    def stage_copy(piece, t):
        source, column = weights(piece, t)
        return pltpu.make_async_copy(
            source.at[part_rows, pl.ds(column, HD)],
            stage.at[piece, t],
            stage_sem.at[piece],
        )

    for piece in range(pieces):
        for t in range(A):
            stage_copy(piece, t).start()

            @pl.when(c == t)
            def _():
                own_copy(piece, t).start()

    table_copies = [
        pltpu.make_async_copy(source, into, table_sem.at[i])
        for i, (source, into) in enumerate(
            ((order_in, order_ref), (docs_in, docs_ref), (owner_in, owner_ref))
        )
    ]
    for copy in table_copies:
        copy.start()

    pl.semaphore_wait(barrier, len(peers))

    targets = ((c, far), (across, quad[2]), (across_z, quad[1]), (across_y, quad[0]))

    for piece in range(pieces):
        pltpu.make_async_copy(stage.at[piece], stage.at[piece], stage_sem.at[piece]).wait()

    def first_send(piece, i):
        t, device = targets[i]
        remote(
            stage.at[piece, t],
            w_at(piece, q, x),
            init_send.at[piece],
            w_recv.at[piece, q],
            device,
        ).start()

    def arrive(piece, source):
        ref = w_at(piece, source, x)
        remote(ref, ref, init_send.at[0], w_recv.at[piece, source], sibling).wait_recv()

    def relay(piece, source, ssem, rsem, device):
        ref = w_at(piece, source, x)
        return remote(ref, ref, ssem, rsem, device)

    def some_rows(piece, count):
        return wbuf.at[piece, pl.ds(0, count * Rp)]

    def arrive_pair(piece, group, count):
        ref = some_rows(piece, count)
        remote(ref, ref, init_send.at[0], pair_recv.at[piece, group], sibling).wait_recv()

    near_sources = [g * A + t for t in (across_y, across_z, across)]
    far_sources = [(1 - g) * A + t for t in (c, across_y, across_z, across)]

    def pair_relay(piece, i):
        group = int(piece == pieces - 1 and i >= len(near_sources))
        relay(
            piece,
            (near_sources + far_sources)[i],
            pair_send.at[piece],
            pair_recv.at[piece, group],
            pair,
        ).start()

    def near_arrival(piece, i):
        source = near_sources[i]
        arrive(piece, source)
        relay(piece, source, far_send.at[piece], w_recv.at[piece, source], far).start()
        pair_relay(piece, i)

    def far_arrival(piece, i):
        arrive(piece, far_sources[i])
        pair_relay(piece, len(near_sources) + i)

    def token_rows(side, k):
        return pl.ds(pl.multiple_of(side * half + k * step, step), step)

    def token_copy(block, k, ssem, rsem, device):
        ref = normed.at[block, token_rows(d, k)]
        return remote(ref, ref, ssem, rsem, device)

    def own_copies(k):
        return (
            token_copy(c, k, own_send.at[0], tok_recv.at[0, k], quad[1]),
            token_copy(c, k, own_send.at[1], tok_recv.at[1, k], quad[0]),
            token_copy(c, k, own_send.at[2], sib_recv.at[0], sibling),
        )

    def pass_copy(k):
        return token_copy(across_z, k, pass_send.at[0], tok_recv.at[2, k], quad[0])

    token_blocks = (across_z, across_y, across)

    def share_copy(i, k):
        return token_copy(
            token_blocks[i], k, share_send.at[i], sib_recv.at[0], sibling
        )

    def token_arrival(i, k):
        ref = normed.at[token_blocks[i], token_rows(d, k)]
        remote(ref, ref, own_send.at[0], tok_recv.at[i, k], sibling).wait_recv()
        if i == 0:
            pass_copy(k).start()
        share_copy(i, k).start()

    def normalize(k):
        def block(i, carry):
            span = pl.ds(pl.multiple_of(k * step + i * 16, 16), 16)
            into = pl.ds(pl.multiple_of(d * half + k * step + i * 16, 16), 16)
            inputs = tokraw[span].astype(jnp.float32)
            mean = jnp.mean(inputs * inputs, -1, keepdims=True)
            normed[c, into] = (inputs * lax.rsqrt(mean + 1e-05) * gain[...]).astype(
                jnp.bfloat16
            )
            return carry

        lax.fori_loop(0, step // 16, block, 0)

    lane = lax.broadcasted_iota(jnp.int32, (rows, HD), 1)
    row_id = lax.broadcasted_iota(jnp.int32, (rows, 1), 0)

    def make_tables():
        step_angle = (row_id % blk).astype(jnp.float32) * freq[...]
        step_cos = jnp.cos(step_angle)
        step_sin = jnp.sin(step_angle)
        sign = jnp.where(lane < HD // 2, -1.0, 1.0)
        entry_id = lax.broadcasted_iota(jnp.int32, (A * slots, 1), 0)
        entries = jnp.zeros((A * slots, 1), jnp.int32)
        for k in range(A * slots):
            entries = jnp.where(entry_id == k, order_ref[g * A * slots + k], entries)
        base_angle = (entries * blk).astype(jnp.float32) * freq[...]
        base_cos = jnp.cos(base_angle)
        base_sin = jnp.sin(base_angle)
        for b in range(A):
            row_cos = jnp.broadcast_to(base_cos[b * slots : b * slots + 1], (rows, HD))
            row_sin = jnp.broadcast_to(base_sin[b * slots : b * slots + 1], (rows, HD))
            for i in range(1, slots):
                k = b * slots + i
                row_cos = jnp.where(row_id // blk == i, base_cos[k : k + 1], row_cos)
                row_sin = jnp.where(row_id // blk == i, base_sin[k : k + 1], row_sin)
            csbuf[0, b] = row_cos * step_cos - row_sin * step_sin
            csbuf[1, b] = (row_sin * step_cos + row_cos * step_sin) * sign

    def make_bias():
        key_id = lax.broadcasted_iota(jnp.int32, (1, T), 1)
        key_pos = jnp.zeros((1, T), jnp.int32)
        key_doc = jnp.zeros((1, T), jnp.int32)
        for i in range(T // blk):
            here = key_id // blk == i
            natural = order_ref[i]
            key_pos = jnp.where(here, natural * blk, key_pos)
            key_doc = jnp.where(here, docs_ref[natural], key_doc)
        key_pos = key_pos + key_id % blk

        def block(b, carry):
            first = jnp.zeros((rows, 1), jnp.int32)
            document = jnp.zeros((rows, 1), jnp.int32)
            for i in range(slots):
                natural = order_ref[(g * A + b) * slots + i]
                here = row_id // blk == i
                first = jnp.where(here, natural * blk, first)
                document = jnp.where(here, docs_ref[natural], document)
            allowed = (key_pos <= first + row_id % blk) & (key_doc == document)
            bias[b] = jnp.where(allowed, 0.0, -jnp.inf)
            return carry

        lax.fori_loop(0, A, block, 0)

    def pick_copies():
        mine = heads // 2
        count = picked.shape[1]
        into = pl.ds(pl.multiple_of(d * count, count), count)
        return (
            pltpu.make_async_copy(picked.at[0], cache_ref.at[into], cache_sem.at[0]),
            remote(
                picked.at[1], cache_ref.at[into], cache_sem.at[1], cache_sem.at[2], sibling
            ),
        )

    def pick_heads():
        prev_copy.wait()
        mine = heads // 2
        group = HD
        taken = group // 2
        out_id = lax.broadcasted_iota(jnp.int32, (taken, group), 0)
        in_id = lax.broadcasted_iota(jnp.int32, (taken, group), 1)
        for side in range(2):
            other = d if side == 0 else 1 - d
            wanted = jnp.zeros((taken, group), jnp.int32)
            for s in range(mine):
                wanted = jnp.where(out_id % mine == s, owner_ref[other * mine + s], wanted)
            chosen = (out_id // mine == in_id // heads) & (in_id % heads == wanted)
            selector = jnp.where(chosen, 1.0, 0.0).astype(jnp.bfloat16)
            for i in range(prev.shape[0] // group):
                picked[side, i * taken : (i + 1) * taken] = jnp.dot(
                    selector,
                    prev[i * group : (i + 1) * group],
                    preferred_element_type=jnp.float32,
                ).astype(jnp.bfloat16)
        for copy in pick_copies():
            copy.start()

    def turn(v, b):
        return v * csbuf[0, b] + pltpu.roll(v, HD // 2, 1) * csbuf[1, b]

    def kv_copy(n, side, b, device):
        ref = kvbuf.at[y, side * A + b]
        rsem = kv_recv.at[b] if n == 1 else kv_recv.at[A + n // 2]
        return remote(ref, ref, kv_send.at[n], rsem, device)

    def kv_arrivals(n):
        if n == 1:
            for b in range(A):
                ref = kvbuf.at[y, (1 - g) * A + b]
                remote(ref, ref, kv_send.at[0], kv_recv.at[b], sibling).wait_recv()
                kv_copy(2, 1 - g, b, quad[0]).start()
        else:
            side = g if n == 0 else 1 - g
            ref = kvbuf.at[1 - y, pl.ds(pl.multiple_of(side * A, A), A)]
            remote(
                ref, ref, kv_send.at[0], kv_recv.at[A + n // 2], sibling
            ).wait_recv()

    def project_kv(b, carry):
        raw = jnp.dot(normed[b], wbuf[0], preferred_element_type=jnp.float32)
        kvbuf[y, g * A + b] = jnp.where(y == 0, turn(raw, b), raw).astype(jnp.bfloat16)
        kv_copy(1, g, b, far).start()
        kv_copy(0, g, b, quad[0]).start()
        return carry

    def span_of(source, part):
        return pl.ds(pl.multiple_of(source * R + part * Rp, Rp), Rp)

    def partial(piece, b, spans):
        total = None
        for span in spans:
            term = jnp.dot(
                normed[b, :, span], wbuf[piece, span], preferred_element_type=jnp.float32
            )
            total = term if total is None else total + term
        return total

    scale = 1.0 / math.sqrt(HD)

    def att_copy(h, b):
        cols = pl.ds(pl.multiple_of((c * hpg + h) * HD, HD), HD)
        return remote(
            att.at[h, b],
            out_ref.at[:, cols],
            att_send.at[h],
            att_recv.at[0],
            dev(x, g * A + b, d),
        )

    def own_out(h):
        cols = pl.ds(pl.multiple_of((c * hpg + h) * HD, HD), HD)
        return pltpu.make_async_copy(att.at[h, c], out_ref.at[:, cols], out_sem.at[h])

    def order(s):
        back = A - 1 - s
        return near(back // 2, back % 2)

    def attend(h, blocks, queries, push=True):
        scores = lax.dot_general(
            jnp.concatenate(queries, 0),
            kvbuf[0].reshape(T, HD),
            (((1,), (1,)), ((), ())),
            preferred_element_type=jnp.float32,
        ) * scale + jnp.concatenate([bias[b] for b in blocks], 0)
        weights = jnp.exp(scores - jnp.max(scores, -1, keepdims=True))
        total = jnp.sum(weights, -1, keepdims=True)
        weighted = jnp.dot(
            weights.astype(jnp.bfloat16),
            kvbuf[1].reshape(T, HD),
            preferred_element_type=jnp.float32,
        )
        done = (weighted / total).astype(jnp.bfloat16)
        for i, b in enumerate(blocks):
            att[h, b] = done[i * rows : (i + 1) * rows]
        if push:
            for b in blocks:
                att_copy(h, b).start()

    def attend_all(h, query):
        blocks = [across, across_z]
        attend(h, blocks, [query(b) for b in blocks])
        attend(h, [across_y], [query(across_y)])
        attend(h, [c], [query(c)], False)
        own_out(h).start()

    def own_tokens(k):
        if k == plan[0]:
            tok_copy.wait()
            gain_copy.wait()
        normalize(k)
        for copy in own_copies(k):
            copy.start()

    def spare(i):
        if i == first_spare:
            for copy in table_copies:
                copy.wait()
        if i:
            make_bias()
            pick_heads()
        else:
            freq_copy.wait()
            make_tables()

    def start_keys():
        ref = normed.at[pl.ds(0, A // 2)]
        remote(ref, ref, own_send.at[0], sib_recv.at[0], sibling).wait_recv()
        for piece in range(pieces):
            pltpu.make_async_copy(
                own_rows(piece), own_rows(piece), local_sem.at[piece]
            ).wait()
        arrive_pair(0, 0, len(near_sources) + len(far_sources))
        lax.fori_loop(0, A, project_kv, 0)

    def project_first():
        arrive_pair(1, 0, near_count + far_count)
        late = [span_of(source, 1 - x) for source in near_sources + far_sources]

        def project(s, carry):
            b = order(s)
            product = acc[0, b] + partial(1, b, late)
            qbuf[b] = turn(product, b).astype(jnp.bfloat16)
            return carry

        lax.fori_loop(0, A, project, 0)

    def attend_first():
        attend_all(0, lambda b: qbuf[b])

    last = hpg
    near_count, far_count = len(near_sources), len(far_sources)

    def project_early(piece, group):
        if group:
            spans = [span_of(source, x) for source in far_sources]
        else:
            spans = [span_of(q, 0), span_of(q, 1)]
            spans += [span_of(source, x) for source in near_sources]

        def project(b, carry):
            term = partial(piece, b, spans)
            acc[piece - 1, b] = acc[piece - 1, b] + term if group else term
            return carry

        lax.fori_loop(0, A, project, 0)

    def attend_last():
        arrive_pair(last, 0, near_count)
        middle = [span_of(source, 1 - x) for source in near_sources]

        def project(b, carry):
            acc[last - 1, b] += partial(last, b, middle)
            return carry

        lax.fori_loop(0, A, project, 0)
        arrive_pair(last, 1, far_count)
        late = [span_of(source, 1 - x) for source in far_sources]

        def query(b):
            return turn(acc[last - 1, b] + partial(last, b, late), b).astype(jnp.bfloat16)

        attend_all(1, query)

    steps = {
        "first": first_send,
        "near": near_arrival,
        "far": far_arrival,
        "own": own_tokens,
        "tok": token_arrival,
        "spare": spare,
        "keys": start_keys,
        "kv": kv_arrivals,
        "query": project_first,
        "head": attend_first,
        "early": project_early,
        "last": attend_last,
    }
    first_spare = [where[0] for name, *where in plan[1] if name == "spare"][0]
    for name, *where in plan[1]:
        steps[name](*where)

    def drain(ref, sem):
        remote(ref, ref, sem, w_recv.at[0, q], far).wait_send()

    for piece in range(pieces):
        drain(some_rows(piece, A), init_send.at[piece])
        drain(some_rows(piece, near_count), far_send.at[piece])
        drain(some_rows(piece, near_count + far_count), pair_send.at[piece])
    half_rows = normed.at[0, pl.ds(0, half)]
    for sem in (*(own_send.at[i] for i in range(3)), pass_send.at[0]):
        drain(half_rows, sem)
    for i in range(len(token_blocks)):
        drain(half_rows, share_send.at[i])
    for n in range(3):
        drain(kvbuf.at[0, pl.ds(0, A)], kv_send.at[n])
    local_pick, sent_pick = pick_copies()
    local_pick.wait()
    sent_pick.wait()
    for h in range(hpg):
        own_out(h).wait()
        drain(att.at[h, pl.ds(0, A - 1)], att_send.at[h])
    ref = kvbuf.at[0, pl.ds(0, hpg * (A - 1))]
    remote(ref, ref, own_send.at[0], att_recv.at[0], sibling).wait_recv()


def quad_plan(
    tokens, norm_gain, w_query, w_key, w_value, block_order, block_docs, head_owner, prev_kv
):
    n_seq = lax.axis_size("seq")
    rows, width = tokens.shape
    R = w_query.shape[0]
    local_kv = w_key.shape[1] // HD
    local_heads = w_query.shape[1] // HD
    A = 2 * local_kv
    hpg = local_heads // A
    slots = block_order.shape[0] // n_seq
    blk = rows // slots
    T = n_seq * rows
    owned = [where[0] for name, *where in PLAN if name == "own"]
    first_own, chunks = owned[0], len(owned)
    kept, planes, heads, _ = prev_kv.shape
    count = kept * planes * (heads // 2)
    frequency = 500000.0 ** (-np.arange(HD // 2, dtype=np.float64) / (HD // 2))
    freq = np.concatenate([frequency, frequency]).astype(np.float32)[None, :]
    sizes = (A, rows, R, hpg, slots, blk, T, chunks, heads)
    pieces = hpg + 1
    dma = pltpu.SemaphoreType.DMA
    anywhere = pl.BlockSpec(memory_space=pl.ANY)
    bf16, f32 = jnp.bfloat16, jnp.float32
    attended, cache = pl.pallas_call(
        functools.partial(quad_kernel, (first_own, PLAN), sizes),
        out_shape=(
            pltpu.VMEM((rows, local_heads * HD), bf16),
            pltpu.VMEM((2 * count, HD), prev_kv.dtype),
        ),
        in_specs=[anywhere] * 10,
        out_specs=(anywhere, anywhere),
        scratch_shapes=[
            pltpu.SMEM(block_order.shape, jnp.int32),
            pltpu.SMEM(block_docs.shape, jnp.int32),
            pltpu.SMEM(head_owner.shape, jnp.int32),
            pltpu.VMEM((pieces, A, R // 2, HD), bf16),
            pltpu.VMEM((1, HD), f32),
            pltpu.VMEM((1, width), f32),
            pltpu.VMEM((rows // 2, width), bf16),
            pltpu.VMEM((pieces, width, HD), bf16),
            pltpu.VMEM((A, rows, width), bf16),
            pltpu.VMEM((A, rows, HD), bf16),
            pltpu.VMEM((hpg, A, rows, HD), f32),
            pltpu.VMEM((2, n_seq, rows, HD), bf16),
            pltpu.VMEM((2, A, rows, HD), f32),
            pltpu.VMEM((A, rows, T), f32),
            pltpu.VMEM((hpg, A, rows, HD), bf16),
            pltpu.VMEM((kept * planes * heads, HD), bf16),
            pltpu.VMEM((2, count, HD), bf16),
            dma((pieces + 4,)),
            dma((pieces,)),
            dma((3,)),
            dma((pieces,)),
            dma((pieces,)),
            dma((pieces,)),
            dma((pieces, n_seq)),
            dma((pieces, 2)),
            dma((3,)),
            dma((1,)),
            dma((3,)),
            dma((3, chunks)),
            dma((1,)),
            dma((3,)),
            dma((A + 2,)),
            dma((hpg,)),
            dma((1,)),
            dma((hpg,)),
            dma((3,)),
        ],
        compiler_params=pltpu.CompilerParams(collective_id=1, has_side_effects=True),
    )(
        block_order,
        block_docs,
        head_owner,
        freq,
        norm_gain[None, :],
        tokens,
        w_query,
        w_key,
        w_value,
        prev_kv.reshape(kept * planes * heads, HD),
    )
    return attended, cache.reshape(2 * kept, planes, heads // 2, HD)


def solution(mesh):
    in_specs = (
        P(("groups", "seq"), None),
        P(),
        P("seq", "dec"),
        P("seq", "dec"),
        P("seq", "dec"),
        P("groups"),
        P("groups"),
        P("groups"),
        P(("groups", "seq", "dec"), None, None, None),
    )
    out_specs = (P(("groups", "seq"), "dec"), P(("groups", "seq"), None, "dec", None))
    X = mesh.shape["groups"]
    n_seq = mesh.shape["seq"]

    def per_device(tokens, norm_gain, w_query, w_key, w_value, *rest):
        A = 2 * (w_key.shape[1] // HD)
        heads = w_query.shape[1] // HD
        fits = (
            mesh.shape["dec"] == 2
            and A & (A - 1) == 0
            and n_seq % A == 0
            and heads % A == 0
            and w_query.shape[0] % (16 * X) == 0
            and tokens.shape[0] % 32 == 0
        )
        squared = (
            fits
            and A == 4
            and X == 2
            and n_seq == 2 * A
            and heads == 2 * A
            and tokens.shape[0] % 128 == 0
            and rest[-1].shape[3] == HD
            and HD % (2 * rest[-1].shape[2]) == 0
            and (rest[-1].shape[0] * rest[-1].shape[1] * rest[-1].shape[2]) % HD == 0
        )
        plan = functools.partial(column_plan, X) if fits else general_plan
        plan = quad_plan if squared else plan
        return plan(tokens, norm_gain, w_query, w_key, w_value, *rest)

    return jax.shard_map(
        per_device, mesh=mesh, in_specs=in_specs, out_specs=out_specs, check_vma=False
    )
```
